128 devices in a mesh: node: 8 (over x, core), local: 16 (over y, z).
Axes of the slice: x: 4, y: 4, z: 4, core: 2. Of those that a mesh axis runs over, the one named last changes fastest.
Arguments:
- tokens: bfloat16 [2048, 7168], P('node', 'local'), may hold values from -6 to 6
- grad_out: bfloat16 [2048, 7168], P('node', 'local'), may hold values from -0.59765625 to 0.59765625
- gates: bfloat16 [2048, 8], P('node'), may hold values from 0.05 to 10
- routes: int32 [2048, 8], P('node'), may hold values from 0 to 31, all different within a row; in each aligned block of 256 rows (0 to 255, 256 to 511, ...) at most 80 rows name the same one
- w_gate: bfloat16 [32, 7168, 1024], P('node', 'local'), may hold values from -0.09375 to 0.09375
- w_up: bfloat16 [32, 7168, 1024], P('node', 'local'), may hold values from -0.09375 to 0.09375
- w_down: bfloat16 [32, 1024, 7168], P('node', None, 'local'), may hold values from -0.25 to 0.25
Outputs:
- grad_tokens: bfloat16 [2048, 7168], P('node', 'local')
- grad_gates: bfloat16 [2048, 8], P('node')
- grad_w_gate: bfloat16 [32, 7168, 1024], P('node', 'local')
- grad_w_up: bfloat16 [32, 7168, 1024], P('node', 'local')
- grad_w_down: bfloat16 [32, 1024, 7168], P('node', None, 'local')
- loads: float32 [32], replicated
The draws below stay inside these ranges and needn't reach their ends.
Inputs may be any that keep to these rules, and one draw needn't show every extreme that they name: `routes`: each row names 8 different experts. Within each aligned block of 256 rows (the rows of one index of node) no expert is named by more than 80 rows, and in some blocks one expert is named by exactly 80 rows.
All inputs are finite; a program needn't handle non-finite values.
Results may differ from the reference program's by a relative error of at most 0.033.
Values may be sent and summed in bfloat16 or wider, within the bound.
A program may use at most 128 MiB of HBM per device.

```python
import math
import jax
import jax.numpy as jnp
import numpy as np
from jax import lax

D = 7168
H = 1024
TOP = 8
TOK_NODE = 256
EXPERTS = 32
CAP = 80
TOKENS = 2048
N_NODE = 8
N_LOCAL = 16


def draw_gates(key, part):
    block_count = TOKENS // TOK_NODE
    block_ids = (jnp.arange(TOKENS, dtype=jnp.int32) // TOK_NODE).astype(jnp.float32)
    frac = block_ids / max(block_count - 1, 1)
    logs = jax.random.uniform(key, (TOKENS, TOP), jnp.float32, jnp.log(0.05), 0.0)
    base = jnp.exp(logs)
    scale = jnp.exp(frac * jnp.log(10.0))
    values = jnp.clip(base * scale[:, None], 0.05, 10.0)
    return values.astype(jnp.bfloat16)


def strengthened(values, rng, source, target, shards_of, factor):
    def block_of(dim):
        return (jnp.arange(values.shape[dim]) // (values.shape[dim] // shards_of)).reshape((-1,) + (1,) * (values.ndim - 1 - dim))

    first = jax.random.permutation(rng, shards_of)[block_of(target)]
    second = (block_of(target) + shards_of // 2) % shards_of
    return jnp.where((block_of(source) == first) | (block_of(source) == second), factor * values, values)


def block_scale(own_key, dims, cuts, smallest, high):
    level, own = 1.0, jax.random.fold_in(own_key, 6)
    for dim, shards_of in cuts:
        draws = jnp.exp(jax.random.uniform(jax.random.fold_in(own, dim), (shards_of,), jnp.float32, smallest / len(cuts), high / len(cuts)))
        level = level * jnp.repeat(draws, dims[dim] // shards_of).reshape([-1 if axis == dim else 1 for axis in range(len(dims))])
    return level


def deal_out(stream_key, own, number, rows, amount, top, most, slope):
    order = jax.random.permutation(stream_key, amount)
    crowded, usual = portions_of(amount, rows * top, most, slope, True), portions_of(amount, rows * top, most, slope, False)
    places = jnp.arange(amount)

    def named(sizes, rotation):
        used = int((sizes > 0).sum())
        fixed = max(1, used // 4)
        shifted = fixed + (places - fixed + rotation * (used - fixed)) % max(1, amount - fixed)
        return jnp.zeros((amount,), jnp.int32).at[order[jnp.where(places < fixed, places, shifted)]].set(jnp.asarray(sizes, jnp.int32))

    sizes = jnp.where(number % 4 == 0, named(crowded, number // 4), named(usual, number - number // 4 - 1))
    mixed = jax.random.permutation(jax.random.fold_in(own, 3), amount)
    source_of, receiver = mixed[0:amount // 2 * 2:2], mixed[1:amount // 2 * 2:2]
    room = jnp.minimum(sizes[source_of] - 1, most - sizes[receiver]) // 2
    room = jnp.where((source_of == order[0]) | (receiver == order[0]) | (sizes[receiver] == 0), 0, jnp.maximum(room, 0))
    shifted = jax.random.randint(jax.random.fold_in(own, 4), (amount // 2,), 0, 1 << 20) % (room + 1)
    sizes = sizes.at[source_of].add(-shifted).at[receiver].add(shifted)
    labels = jnp.searchsorted(jnp.cumsum(sizes), jnp.arange(rows * top), side="right").astype(jnp.int32)
    grid = labels.reshape(top, rows).T
    grid = grid[jax.random.permutation(jax.random.fold_in(own, 1), rows)]
    rotation = jax.random.randint(jax.random.fold_in(own, 2), (rows, 1), 0, top)
    return jnp.take_along_axis(grid, (jnp.arange(top)[None, :] + rotation) % top, axis=1)


def portions_of(amount, total, reach, lean, full):
    weights = [(1 << 20) // math.isqrt(rank ** lean) + 1 for rank in range(1, amount + 1)]
    largest = reach if full else min(reach, max(-(-total // amount), total * weights[0] // sum(weights)))
    least = 1 if total - largest >= amount - 1 else 0
    holding, rest = [largest] + [least] * (amount - 1), total - largest - least * (amount - 1)
    while rest > 0:
        movable = [i for i in range(1, amount) if holding[i] < largest] or [i for i in range(1, amount) if holding[i] < reach]
        mass, remaining = sum([weights[i] for i in movable]), rest
        for i in movable:
            more = min(reach - holding[i], max(1, remaining * weights[i] // mass), rest)
            holding[i] = holding[i] + more
            rest = rest - more
    return np.array(holding)


def bell_draw(key, dims, scale, bound, split=(), kind=jnp.bfloat16):
    factor_of = block_scale(key, dims, split, -0.22, 0.18) if split else 1.0
    result = jax.random.normal(key, dims, jnp.float32) * scale * factor_of
    return jnp.minimum(jnp.maximum(result, -bound), bound).astype(kind)


def gaussian_with(key, shape, deviation, most, cuts, heavy, kind=jnp.bfloat16):
    entries = deviation * jax.random.normal(key, shape, jnp.float32)
    if cuts:
        entries = entries * block_scale(key, shape, cuts, -0.22, 0.18)
    return jnp.clip(strengthened(entries, jax.random.fold_in(key, 3), *heavy), -most, most).astype(kind)


def setup_inputs(seed: int = 0) -> dict:
    seeds = jax.random.split(jax.random.key(seed), 8)
    tokens = bell_draw(seeds[0], (TOKENS, D), 1.0, 6.0, ((0, 8), (1, 16)))
    grad_out = bell_draw(seeds[1], (TOKENS, D), 0.1, 0.59765625, ((0, 8), (1, 16)))
    gates = draw_gates(jax.random.fold_in(seeds[7], 71), 0)
    routes_keys = jax.random.split(jax.random.fold_in(seeds[3], 1), TOKENS // TOK_NODE)
    routes_turns = jax.random.permutation(jax.random.fold_in(seeds[3], 3), TOKENS // TOK_NODE)
    routes = jax.vmap(lambda own, number: deal_out(jax.random.fold_in(seeds[3], 2), own, number, TOK_NODE, EXPERTS, TOP, CAP, 2))(routes_keys, routes_turns).reshape((TOKENS, TOP))
    w_gate = gaussian_with(seeds[4], (EXPERTS, D, H), D ** -0.5, 0.09375, ((0, 8), (1, 16)), (1, 2, 16, 2.0))
    w_up = gaussian_with(seeds[5], (EXPERTS, D, H), D ** -0.5, 0.09375, ((0, 8), (1, 16)), (1, 2, 16, 2.0))
    w_down = gaussian_with(seeds[6], (EXPERTS, H, D), H ** -0.5, 0.25, ((0, 8), (2, 16)), (2, 1, 16, 2.0))
    return {"tokens": tokens, "grad_out": grad_out, "gates": gates, "routes": routes, "w_gate": w_gate, "w_up": w_up, "w_down": w_down}


def activation_grads(gate_pre, up_pre, back_hidden, gate_col):
    logistic = jax.nn.sigmoid(gate_pre)
    swished = gate_pre * logistic
    hidden = swished * up_pre
    products = jnp.sum(hidden * back_hidden, axis=-1)
    weight_col = gate_col.astype(jnp.float32)
    scaled = weight_col * back_hidden
    grad_up = (scaled * swished).astype(jnp.bfloat16)
    grad_gate = (scaled * up_pre * logistic * (1.0 + gate_pre * (1.0 - logistic))).astype(jnp.bfloat16)
    weighted = (weight_col * hidden).astype(jnp.bfloat16)
    return weighted, grad_gate, grad_up, products


def slot_tables(flat_routes, expert_count, capacity):
    experts_row = jnp.arange(expert_count, dtype=jnp.int32)
    onehot = (flat_routes[..., None] == experts_row).astype(jnp.int32)
    before = jnp.cumsum(onehot, axis=-2) - onehot
    slot_index = jnp.sum(before * onehot, axis=-1)
    target = flat_routes * capacity + slot_index
    return target


def weight_loads(flat_routes, flat_gates, expert_count):
    experts_row = jnp.arange(expert_count, dtype=jnp.int32)
    onehot = (flat_routes[:, None] == experts_row).astype(jnp.float32)
    return jnp.sum(onehot * flat_gates.astype(jnp.float32)[:, None], axis=0)


def group_sum(partials):
    rounded = lax.optimization_barrier(partials.astype(jnp.bfloat16))
    return jnp.sum(rounded.astype(jnp.float32), axis=0)


def reference(tokens, grad_out, gates, routes, w_gate, w_up, w_down):
    blocks = routes.reshape(N_NODE, TOK_NODE * TOP)
    target = slot_tables(blocks, EXPERTS, CAP)
    weight_sum = weight_loads(routes.reshape(-1), gates.reshape(-1), EXPERTS)
    block_ids = jnp.arange(N_NODE, dtype=jnp.int32)[:, None]
    owners = jnp.broadcast_to(jnp.arange(TOK_NODE * TOP, dtype=jnp.int32)[None, :] // TOP, target.shape)
    token_of = jnp.full((N_NODE, EXPERTS * CAP), TOK_NODE, jnp.int32).at[block_ids, target].set(owners)
    gate_of = jnp.zeros((N_NODE, EXPERTS * CAP), jnp.bfloat16).at[block_ids, target].set(gates.reshape(N_NODE, TOK_NODE * TOP))
    zero_rows = jnp.zeros((N_NODE, 1, D), jnp.bfloat16)
    padded_tokens = jnp.concatenate([tokens.reshape(N_NODE, TOK_NODE, D), zero_rows], axis=1)
    padded_grads = jnp.concatenate([grad_out.reshape(N_NODE, TOK_NODE, D), zero_rows], axis=1)
    group_width = D // N_LOCAL
    slot_rows = N_NODE * CAP

    def one_expert(expert):
        start = (expert * CAP).astype(jnp.int32)
        row_ids = lax.dynamic_slice_in_dim(token_of, start, CAP, 1)
        gate_col = lax.dynamic_slice_in_dim(gate_of, start, CAP, 1).reshape(slot_rows, 1)
        token_rows = padded_tokens[block_ids, row_ids].reshape(slot_rows, D)
        grad_rows = padded_grads[block_ids, row_ids].reshape(slot_rows, D)
        gate_matrix = w_gate[expert]
        up_matrix = w_up[expert]
        down_matrix = w_down[expert]
        token_groups = token_rows.reshape(slot_rows, N_LOCAL, group_width).astype(jnp.float32)
        grad_groups = grad_rows.reshape(slot_rows, N_LOCAL, group_width).astype(jnp.float32)
        gate_groups = gate_matrix.reshape(N_LOCAL, group_width, H).astype(jnp.float32)
        up_groups = up_matrix.reshape(N_LOCAL, group_width, H).astype(jnp.float32)
        down_groups = down_matrix.reshape(H, N_LOCAL, group_width).astype(jnp.float32)
        gate_pre = group_sum(jnp.einsum("rld,ldh->lrh", token_groups, gate_groups, precision=lax.Precision.HIGHEST))
        up_pre = group_sum(jnp.einsum("rld,ldh->lrh", token_groups, up_groups, precision=lax.Precision.HIGHEST))
        back_hidden = group_sum(jnp.einsum("rld,hld->lrh", grad_groups, down_groups, precision=lax.Precision.HIGHEST))
        weighted, grad_gate, grad_up, products = activation_grads(gate_pre, up_pre, back_hidden, gate_col)
        input_rows = (jnp.dot(grad_gate, gate_matrix.T, preferred_element_type=jnp.float32)
                      + jnp.dot(grad_up, up_matrix.T, preferred_element_type=jnp.float32)).astype(jnp.bfloat16)
        grad_wg = jnp.dot(token_rows.T, grad_gate, preferred_element_type=jnp.float32).astype(jnp.bfloat16)
        grad_wu = jnp.dot(token_rows.T, grad_up, preferred_element_type=jnp.float32).astype(jnp.bfloat16)
        grad_wd = jnp.dot(weighted.T, grad_rows, preferred_element_type=jnp.float32).astype(jnp.bfloat16)
        return (input_rows.reshape(N_NODE, CAP, D), products.astype(jnp.bfloat16).reshape(N_NODE, CAP),
                grad_wg, grad_wu, grad_wd)

    input_rows, products, grad_wg, grad_wu, grad_wd = lax.map(one_expert, jnp.arange(EXPERTS, dtype=jnp.int32))
    returned_rows = jnp.transpose(input_rows, (1, 0, 2, 3)).reshape(N_NODE, EXPERTS * CAP, D)
    returned_products = jnp.transpose(products, (1, 0, 2)).reshape(N_NODE, EXPERTS * CAP)
    picked = returned_rows[block_ids, target].reshape(N_NODE, TOK_NODE, TOP, D)
    grad_tokens = jnp.sum(picked.astype(jnp.float32), axis=2).astype(jnp.bfloat16).reshape(N_NODE * TOK_NODE, D)
    grad_gates = returned_products[block_ids, target].reshape(N_NODE * TOK_NODE, TOP)
    loads = weight_sum * (EXPERTS / (TOK_NODE * TOP))
    return grad_tokens, grad_gates, grad_wg, grad_wu, grad_wd, loads
```

```python
import jax
import jax.numpy as jnp
from jax import lax
from jax.experimental import pallas as pl
from jax.experimental.pallas import tpu as pltpu
from jax.sharding import PartitionSpec as P

BF = jnp.bfloat16
F32 = jnp.float32
MESH = pl.DeviceIdType.MESH
FEAT, TOK, HID, CAPS, EXP = 448, 256, 1024, 80, 4
PAIR = 2 * TOK
ROWS = 2 * CAPS
HALF = HID // 2
BLK = 2 * FEAT + 16
CROWS = FEAT + 16
CUT = 240
ALL_EXPERTS = 32


def dot_t(a, b):
    return lax.dot_general(a, b, (((1,), (1,)), ((), ())), preferred_element_type=F32)


def dot_n(a, b):
    return jnp.dot(a, b, preferred_element_type=F32)


def add2(a, b):
    return (a.astype(F32) + b.astype(F32)).astype(BF)


def add3(a, b, c):
    return a.astype(F32) + b.astype(F32) + c.astype(F32)


def kernel(
    meta_h, tok_h, dy_h, wg_h, wu_h, wd_h,
    gt_h, gg_h, load_h, og_h, ou_h, od_h,
    wt, gat, tri, hot, slot, prt, r1a, r1b, r2a, r2b, sa, sb, r3a, r3b, r4a, r4b,
    act, dv, dr, df, acc, bk, cb, c1r, cs, c2a, c2b, c3r, gt, gg, ld,
    lsem, ssem, rsem, dsem, esem,
):
    node, local = lax.axis_index("node"), lax.axis_index("local")
    x, c = node // 2, node % 2
    y, z = local // 4, local % 4
    yp, ym, y2 = (y + 1) % 4, (y + 3) % 4, (y + 2) % 4
    zp, zm, z2 = (z + 1) % 4, (z + 3) % 4, (z + 2) % 4

    def at_x(k):
        return (((x + k) % 4) * 2 + c, local)

    def at_yz(a, b):
        return (node, a * 4 + b)

    mate = (x * 2 + 1 - c, local)
    xpd, xmd = at_x(1), at_x(3)
    ypd, ymd, zpd, zmd = at_yz(yp, z), at_yz(ym, z), at_yz(y, zp), at_yz(y, zm)
    d_z1, d_z3 = at_yz(y, z + 1 - 2 * (z % 2)), at_yz(y, 3 - z)
    d_y1, d_y3 = at_yz(y + 1 - 2 * (y % 2), z), at_yz(3 - y, z)

    def rc(src, dst, k, dev):
        return pltpu.make_async_remote_copy(
            src_ref=src, dst_ref=dst, send_sem=ssem.at[k], recv_sem=rsem.at[k],
            device_id=dev, device_id_type=MESH,
        )

    def go(copies):
        for cp in copies:
            cp.start()

    def done(copies):
        for cp in copies:
            cp.wait()

    def lane(q, base):
        return pl.ds(pl.multiple_of(base + 128 * q, 128), 128)

    lo, hi = pl.ds(0, CAPS), pl.ds(CAPS, CAPS)
    left, right = pl.ds(0, TOK), pl.ds(TOK, TOK)
    ca = pl.ds(0, HALF)

    own = [
        pltpu.make_async_copy(tok_h, gat.at[0, pl.ds(0, FEAT), left], lsem.at[0]),
        pltpu.make_async_copy(dy_h, gat.at[0, pl.ds(FEAT, FEAT), left], lsem.at[1]),
        pltpu.make_async_copy(meta_h, gat.at[0, pl.ds(2 * FEAT, 16), left], lsem.at[2]),
    ]
    go(own)
    weights = [pltpu.make_async_copy(h, wt.at[m], lsem.at[3 + m]) for m, h in enumerate((wg_h, wu_h, wd_h))]
    go(weights)
    barrier = pltpu.get_barrier_semaphore()
    for dev in (mate, xpd, xmd, ypd, ymd, zpd, zmd):
        pl.semaphore_signal(barrier, inc=1, device_id=dev, device_id_type=MESH)
    row_i = lax.broadcasted_iota(jnp.int32, (PAIR, PAIR), 0)
    col_i = lax.broadcasted_iota(jnp.int32, (PAIR, PAIR), 1)
    same = (row_i < TOK) == (col_i < TOK)
    tri[...] = jnp.where((row_i < col_i) & same, 1.0, 0.0).astype(BF)
    done(own)
    pl.semaphore_wait(barrier, 7)
    first = [
        rc(gat.at[0, :, left], gat.at[0, :, right], 36, mate),
        rc(gat.at[0, :, left], gat.at[3, :, left], 37, xpd),
        rc(gat.at[0, :, left], gat.at[1, :, left], 38, xmd),
    ]
    go(first)

    def second():
        return [
            rc(gat.at[3, pl.ds(0, FEAT), left], gat.at[2, pl.ds(0, FEAT), left], 39, xpd),
            rc(gat.at[1, pl.ds(FEAT, BLK - FEAT), left], gat.at[2, pl.ds(FEAT, BLK - FEAT), left], 40, xmd),
            rc(gat.at[3, :, left], gat.at[3, :, right], 41, mate),
            rc(gat.at[1, :, left], gat.at[1, :, right], 42, mate),
        ]

    def third():
        return [rc(gat.at[2, :, left], gat.at[2, :, right], 43, mate)]

    def meta_of(r):
        m = gat[r, pl.ds(2 * FEAT, 16), :].astype(F32)
        return m[:8], m[8:]

    def expert_id(e):
        return (node * EXP + e).astype(F32)

    def project(i):
        r, par = (4 - i) % 4, i % 2
        routes, _ = meta_of(r)
        rid = lax.broadcasted_iota(jnp.int32, (16, PAIR), 0)
        lid = lax.broadcasted_iota(jnp.int32, (16, PAIR), 1)
        member = jnp.zeros((16, PAIR), F32)
        for e in range(EXP):
            one = jnp.sum(jnp.where(routes == expert_id(e), 1.0, 0.0), axis=0, keepdims=True)
            member = jnp.where(rid == e, jnp.broadcast_to(one, (16, PAIR)), member)
        before = dot_n(member.astype(BF), tri[...])
        shift = jnp.where(lid < TOK, 0.0, float(CAPS))
        slot[...] = jnp.where(member > 0.5, before + shift, -1.0)
        sid = lax.broadcasted_iota(jnp.int32, (ROWS, PAIR), 0).astype(F32)

        def one_expert(e, carry):
            o = jnp.where(sid == slot[pl.ds(e, 1), :], 1.0, 0.0).astype(BF)
            hot[r, e] = o
            xr = dot_t(o, gat[r, pl.ds(0, FEAT), :]).astype(BF)
            prt[par, 0, e] = dot_n(xr, wt[0, e]).astype(BF)
            prt[par, 1, e] = dot_n(xr, wt[1, e]).astype(BF)
            dr_ = dot_t(o, gat[r, pl.ds(FEAT, FEAT), :]).astype(BF)
            prt[par, 2, e] = dot_n(dr_, wt[2, e]).astype(BF)
            return carry

        lax.fori_loop(0, EXP, one_expert, 0)

    def s1(i):
        p = prt.at[i % 2]
        return [
            rc(p.at[:, y2, lo, ca], r1a.at[0], 0, ymd),
            rc(p.at[:, y2, hi, ca], r1a.at[1], 1, ypd),
            rc(p.at[:, :, lo, lane(z2, HALF)], r1b.at[0], 2, zmd),
            rc(p.at[:, :, hi, lane(z2, HALF)], r1b.at[1], 3, zpd),
        ]

    def s1_add(i):
        p = prt.at[i % 2]
        for m in range(3):
            p[m, ym, lo, ca] = add2(p[m, ym, lo, ca], r1a[0, m])
            p[m, yp, hi, ca] = add2(p[m, yp, hi, ca], r1a[1, m])
            p[m, :, lo, lane(zm, HALF)] = add2(p[m, :, lo, lane(zm, HALF)], r1b[0, m])
            p[m, :, hi, lane(zp, HALF)] = add2(p[m, :, hi, lane(zp, HALF)], r1b[1, m])

    def s2(i):
        p = prt.at[i % 2]
        return [
            rc(p.at[:, yp, :, ca], r2a.at[0], 4, ypd),
            rc(p.at[:, ym, :, ca], r2a.at[1], 5, ymd),
            rc(p.at[:, :, :, lane(zp, HALF)], r2b.at[0], 6, zpd),
            rc(p.at[:, :, :, lane(zm, HALF)], r2b.at[1], 7, zmd),
        ]

    def s2_add(i):
        p = prt.at[i % 2]
        for m in range(3):
            sa[m] = add3(p[m, y, :, ca], r2a[0, m], r2a[1, m]).astype(BF)
            sb[m] = add3(p[m, :, :, lane(z, HALF)], r2b[0, m], r2b[1, m]).astype(BF)

    def s3():
        return [
            rc(sa.at[:, lo, lane(z2, 0)], r3a.at[0], 8, zmd),
            rc(sa.at[:, hi, lane(z2, 0)], r3a.at[1], 9, zpd),
            rc(sb.at[:, y2, lo], r3b.at[0], 10, ymd),
            rc(sb.at[:, y2, hi], r3b.at[1], 11, ypd),
        ]

    def s3_add():
        for m in range(3):
            sa[m, lo, lane(zm, 0)] = add2(sa[m, lo, lane(zm, 0)], r3a[0, m])
            sa[m, hi, lane(zp, 0)] = add2(sa[m, hi, lane(zp, 0)], r3a[1, m])
            sb[m, ym, lo] = add2(sb[m, ym, lo], r3b[0, m])
            sb[m, yp, hi] = add2(sb[m, yp, hi], r3b[1, m])

    def s4():
        return [
            rc(sa.at[:, :, lane(zp, 0)], r4a.at[0], 12, zpd),
            rc(sa.at[:, :, lane(zm, 0)], r4a.at[1], 13, zmd),
            rc(sb.at[:, yp], r4b.at[0], 14, ypd),
            rc(sb.at[:, ym], r4b.at[1], 15, ymd),
        ]

    def activate(i):
        r, par = (4 - i) % 4, i % 2
        routes, gates = meta_of(r)
        match = jnp.where(routes == expert_id(y), 1.0, 0.0)
        gate_row = jnp.sum(match * gates, axis=0, keepdims=True)
        oh = hot[r, y].astype(F32)
        q = jnp.sum(oh * gate_row, axis=1, keepdims=True)
        dots = jnp.zeros((ROWS, 1), F32)
        for k in range(2):
            if k == 0:
                g, u, b = (add3(sa[m, :, lane(z, 0)], r4a[0, m], r4a[1, m]) for m in range(3))
            else:
                g, u, b = (add3(sb[m, y], r4b[0, m], r4b[1, m]) for m in range(3))
            logistic = 1.0 / (1.0 + jnp.exp(-g))
            swished = g * logistic
            hidden = swished * u
            dots = dots + jnp.sum(hidden * b, axis=1, keepdims=True)
            scaled = q * b
            at = lane(z, k * HALF)
            act[par, 0, y, :, at] = (scaled * u * logistic * (1.0 + g * (1.0 - logistic))).astype(BF)
            act[par, 1, y, :, at] = (scaled * swished).astype(BF)
            act[par, 2, y, :, at] = (q * hidden).astype(BF)
        dv[0] = match * jnp.sum(oh * dots, axis=0, keepdims=True)

    def a1(i):
        t = act.at[i % 2]
        az, bz = t.at[:, y, :, lane(z, 0)], t.at[:, y, :, lane(z, HALF)]
        return [rc(az, az, 16, zpd), rc(az, az, 17, zmd), rc(bz, bz, 18, ypd), rc(bz, bz, 19, ymd),
                rc(dv.at[0], dr.at[0], 32, d_z1)]

    def a2(i):
        t = act.at[i % 2]
        v = [t.at[:, y, lo, lane(zm, 0)], t.at[:, y, hi, lane(zp, 0)],
             t.at[:, ym, lo, lane(z, HALF)], t.at[:, yp, hi, lane(z, HALF)]]
        return [rc(v[0], v[0], 20, zpd), rc(v[1], v[1], 21, zmd), rc(v[2], v[2], 22, ypd), rc(v[3], v[3], 23, ymd),
                rc(dv.at[1], dr.at[1], 33, d_z3)]

    def a3(i):
        t = act.at[i % 2]
        ay, bz = t.at[:, y, :, ca], t.at[:, :, :, lane(z, HALF)]
        return [rc(ay, ay, 24, ypd), rc(ay, ay, 25, ymd), rc(bz, bz, 26, zpd), rc(bz, bz, 27, zmd),
                rc(dv.at[2], dr.at[2], 34, d_y1)]

    def a4(i):
        t = act.at[i % 2]
        v = [t.at[:, ym, lo, ca], t.at[:, yp, hi, ca],
             t.at[:, :, lo, lane(zm, HALF)], t.at[:, :, hi, lane(zp, HALF)]]
        return [rc(v[0], v[0], 28, ypd), rc(v[1], v[1], 29, ymd), rc(v[2], v[2], 30, zpd), rc(v[3], v[3], 31, zmd),
                rc(dv.at[3], dr.at[3], 35, d_y3)]

    def dstep(k):
        dv[k + 1] = dv[k] + dr[k]

    def post_a(j):
        r, par = (4 - j) % 4, j % 2
        bk[...] = jnp.zeros_like(bk)

        def one_expert(e, carry):
            rb = dot_t(wt[0, e], act[par, 0, e]) + dot_t(wt[1, e], act[par, 1, e])
            bk[...] += dot_n(rb.astype(BF), hot[r, e])
            return carry

        lax.fori_loop(0, EXP, one_expert, 0)
        cb[r, pl.ds(0, FEAT), :] = bk[...].astype(BF)
        cb[r, pl.ds(FEAT, 16), :] = jnp.concatenate([df[par], jnp.zeros((8, PAIR), F32)], 0).astype(BF)

    def post_b(j):
        r, par = (4 - j) % 4, j % 2

        def one_expert(e, carry):
            xt = dot_t(gat[r, pl.ds(0, FEAT), :], hot[r, e]).astype(BF)
            acc[0, e] = (acc[0, e].astype(F32) + dot_n(xt, act[par, 0, e])).astype(BF)
            acc[1, e] = (acc[1, e].astype(F32) + dot_n(xt, act[par, 1, e])).astype(BF)
            dt = dot_t(gat[r, pl.ds(FEAT, FEAT), :], hot[r, e]).astype(BF)
            acc[2, e] = (acc[2, e].astype(F32) + dot_n(dt, act[par, 2, e])).astype(BF)
            return carry

        lax.fori_loop(0, EXP, one_expert, 0)

    def c1(r):
        return [pltpu.make_async_remote_copy(
            src_ref=cb.at[r, :, right], dst_ref=c1r.at[r], send_sem=dsem.at[r], recv_sem=esem.at[r],
            device_id=mate, device_id_type=MESH)]

    def c2():
        return [rc(cs.at[2, pl.ds(0, CUT)], c2a, 44, xpd), rc(cs.at[2, pl.ds(CUT, CROWS - CUT)], c2b, 45, xmd)]

    def c3(k):
        return rc(cs.at[1], c3r.at[0], 46, xpd) if k == 0 else rc(cs.at[3], c3r.at[1], 47, xmd)

    done(first[:1])
    done(weights)
    project(jnp.int32(0))
    go(s1(0))

    def body(i, carry):
        rs = i <= 3
        ag = i >= 1

        @pl.when(ag)
        def _():
            go(a1(i - 1))

        @pl.when(i == 1)
        def _():
            done(third())

        @pl.when((i >= 1) & (i <= 2))
        def _():
            project(i + 1)

        @pl.when(ag)
        def _():
            done(a1(i - 1))
            dstep(0)
            go(a2(i - 1))

        @pl.when(rs)
        def _():
            done(s1(i))
            s1_add(i)
            go(s2(i))

        @pl.when(i == 0)
        def _():
            done(first[1:])
            go(second())

            def clear(e, cc):
                for m in range(3):
                    acc[m, e] = jnp.zeros((FEAT, HID), BF)
                return cc

            lax.fori_loop(0, EXP, clear, 0)
            copies = second()
            done(copies[2:])
            project(jnp.int32(1))
            done(copies[:2])
            go(third())

        @pl.when(ag)
        def _():
            done(a2(i - 1))
            dstep(1)
            go(a3(i - 1))

        @pl.when(i >= 2)
        def _():
            post_a(i - 2)
            go(c1((6 - i) % 4))
            post_b(i - 2)

        @pl.when(rs)
        def _():
            done(s2(i))
            s2_add(i)
            go(s3())

        @pl.when(ag)
        def _():
            done(a3(i - 1))
            dstep(2)
            go(a4(i - 1))

        @pl.when(rs)
        def _():
            done(s3())
            s3_add()
            go(s4())

        @pl.when(i <= 2)
        def _():
            go(s1(i + 1))

        @pl.when(rs)
        def _():
            done(s4())
            activate_guard(i)

        @pl.when(i >= 2)
        def _():
            r = (6 - i) % 4
            done(c1(r))
            cs[r] = add2(cb[r, :, left], c1r[r])

        @pl.when(i == 4)
        def _():
            go(c2())

        return carry

    def activate_guard(i):
        @pl.when(i >= 1)
        def _():
            done(a4(i - 1))
            dstep(3)
            df[(i - 1) % 2] = dv[4]

        activate(i)

    lax.fori_loop(0, 5, body, 0)
    done(a4(3))
    dstep(3)
    df[1] = dv[4]
    post_a(3)
    go(c1(1))
    done(c2())
    cs[3, pl.ds(CUT, CROWS - CUT), :] = add2(cs[3, pl.ds(CUT, CROWS - CUT), :], c2b[...])
    c3(1).start()
    done(c1(1))
    cs[1] = add2(cb[1, :, left], c1r[1])
    cs[1, pl.ds(0, CUT), :] = add2(cs[1, pl.ds(0, CUT), :], c2a[...])
    c3(0).start()
    post_b(3)
    outs = [pltpu.make_async_copy(acc.at[m], h, lsem.at[3 + m]) for m, h in enumerate((og_h, ou_h, od_h))]
    go(outs)

    ld[...] = jnp.zeros_like(ld)
    eid = lax.broadcasted_iota(jnp.int32, (ALL_EXPERTS, 128), 0)

    def one_block(b, carry):
        r = (b // 2 - x + 4) % 4
        cc = (b % 2 + c) % 2
        m = gat[r, pl.ds(2 * FEAT, 16), pl.ds(pl.multiple_of(cc * TOK, TOK), TOK)].astype(F32)
        routes, gates = m[:8], m[8:]
        tot = jnp.zeros((ALL_EXPERTS, 128), F32)
        for e in range(ALL_EXPERTS):
            s = jnp.sum(jnp.where(routes == float(e), gates, 0.0), axis=0, keepdims=True)
            s = jnp.sum(s, axis=1, keepdims=True)
            tot = jnp.where(eid == e, jnp.broadcast_to(s, (ALL_EXPERTS, 128)), tot)
        ld[...] += tot
        return carry

    lax.fori_loop(0, 8, one_block, 0)
    ld[...] = ld[...] * (1.0 / 64.0)
    done([c3(0), c3(1)])
    total = add3(cs[0], c3r[0], c3r[1]).astype(BF)
    gt[...] = total[:FEAT]
    gg[...] = total[FEAT:]
    last = [
        pltpu.make_async_copy(gt, gt_h, lsem.at[0]),
        pltpu.make_async_copy(gg, gg_h, lsem.at[1]),
        pltpu.make_async_copy(ld, load_h, lsem.at[2]),
    ]
    go(last)
    done(last)
    done(outs)


def on_device(tokens, grad_out, gates, routes, w_gate, w_up, w_down):
    meta = jnp.concatenate([routes.T.astype(BF), gates.T], 0)
    shape = jax.ShapeDtypeStruct
    any_ = pl.BlockSpec(memory_space=pl.ANY)
    V = pltpu.VMEM
    w_shape = (EXP, FEAT, HID)
    scratch = [
        V((3, *w_shape), BF), V((4, BLK, PAIR), BF), V((PAIR, PAIR), BF), V((4, EXP, ROWS, PAIR), BF),
        V((16, PAIR), F32), V((2, 3, EXP, ROWS, HID), BF),
        V((2, 3, CAPS, HALF), BF), V((2, 3, EXP, CAPS, 128), BF),
        V((2, 3, ROWS, HALF), BF), V((2, 3, EXP, ROWS, 128), BF),
        V((3, ROWS, HALF), BF), V((3, EXP, ROWS, 128), BF),
        V((2, 3, CAPS, 128), BF), V((2, 3, CAPS, 128), BF),
        V((2, 3, ROWS, 128), BF), V((2, 3, ROWS, 128), BF),
        V((2, 3, EXP, ROWS, HID), BF), V((5, 8, PAIR), F32), V((4, 8, PAIR), F32), V((2, 8, PAIR), F32),
        V((3, *w_shape), BF), V((FEAT, PAIR), F32), V((4, CROWS, PAIR), BF), V((4, CROWS, TOK), BF),
        V((4, CROWS, TOK), BF), V((CUT, TOK), BF), V((CROWS - CUT, TOK), BF), V((2, CROWS, TOK), BF),
        V((FEAT, TOK), BF), V((16, TOK), BF), V((ALL_EXPERTS, 128), F32),
        pltpu.SemaphoreType.DMA((6,)), pltpu.SemaphoreType.DMA((48,)), pltpu.SemaphoreType.DMA((48,)),
        pltpu.SemaphoreType.DMA((4,)), pltpu.SemaphoreType.DMA((4,)),
    ]
    gt, gg, ld, og, ou, od = pl.pallas_call(
        kernel,
        name="expert_backward",
        out_shape=(
            shape((FEAT, TOK), BF), shape((16, TOK), BF), shape((ALL_EXPERTS, 128), F32),
            shape(w_shape, BF), shape(w_shape, BF), shape(w_shape, BF),
        ),
        in_specs=[any_] * 6,
        out_specs=[any_] * 6,
        scratch_shapes=scratch,
        compiler_params=pltpu.CompilerParams(
            collective_id=0, has_side_effects=True, vmem_limit_bytes=66_900_000
        ),
    )(meta, tokens.T, grad_out.T, w_gate, w_up, jnp.transpose(w_down, (0, 2, 1)))
    return gt.T, gg[:8].T, og, ou, jnp.transpose(od, (0, 2, 1)), ld[:, 0]


def solution(mesh):
    in_specs = (
        P("node", "local"),
        P("node", "local"),
        P("node", None),
        P("node", None),
        P("node", "local", None),
        P("node", "local", None),
        P("node", None, "local"),
    )
    out_specs = (
        P("node", "local"),
        P("node", None),
        P("node", "local", None),
        P("node", "local", None),
        P("node", None, "local"),
        P(),
    )
    return jax.shard_map(
        on_device, mesh=mesh, in_specs=in_specs, out_specs=out_specs, check_vma=False
    )
```

```python
import jax
import jax.numpy as jnp
from jax import lax
from jax.experimental import pallas as pl
from jax.experimental.pallas import tpu as pltpu
from jax.sharding import PartitionSpec as P

BF = jnp.bfloat16
F32 = jnp.float32
MESH = pl.DeviceIdType.MESH
FEAT, TOK, HID, CAPS, EXP = 448, 256, 1024, 80, 4
PAIR = 2 * TOK
ROWS = 2 * CAPS
NLO = 48
HALF = HID // 2
BLK = 2 * FEAT + 16
CROWS = FEAT + 16
CUT = 240
ALL_EXPERTS = 32


def dot_t(a, b):
    return lax.dot_general(a, b, (((1,), (1,)), ((), ())), preferred_element_type=F32)


def dot_n(a, b):
    return jnp.dot(a, b, preferred_element_type=F32)


def add2(a, b):
    return (a.astype(F32) + b.astype(F32)).astype(BF)


def add3(a, b, c):
    return a.astype(F32) + b.astype(F32) + c.astype(F32)


class Part:
    def __init__(self, r, rows, lanes, local_rows, cut, bufs, base, par, dpar):
        self.r, self.rows, self.lanes, self.n, self.cut = r, rows, lanes, local_rows, cut
        self.width = lanes[1] - lanes[0]
        (self.p, self.r1a, self.r1b, self.r2a, self.r2b, self.sa, self.sb,
         self.r3a, self.r3b, self.r4a, self.r4b, self.t) = bufs
        self.base, self.par, self.d = base, par, dpar
        self.lo, self.hi = pl.ds(0, cut), pl.ds(cut, local_rows - cut)
        self.nlo, self.nhi = pl.ds(0, cut), pl.ds(0, local_rows - cut)
        self.all = pl.ds(0, local_rows)
        self.ln = pl.ds(lanes[0], self.width)
        self.rw = pl.ds(rows[0], local_rows)


def kernel(
    routes_h, gates_h, tok_h, dy_h, wg_h, wu_h, wd_h,
    gt, gg, ld, acc0, acc1, acc2,
    wt, gat, tri, hot, slot, rbuf, gbuf, prt, r1a, r1b, r2a, r2b, sa, sb, r3a, r3b, r4a, r4b, act,
    prt_h, r1a_h, r1b_h, r2a_h, r2b_h, sa_h, sb_h, r3a_h, r3b_h, r4a_h, r4b_h, act_h,
    dv, dr, df, bk, cb, c1r, cs, c2a, c2b, c3r,
    lsem, ssem, rsem,
):
    acc = (acc0, acc1, acc2)
    node, local = lax.axis_index("node"), lax.axis_index("local")
    x, c = node // 2, node % 2
    y, z = local // 4, local % 4
    yp, ym, y2 = (y + 1) % 4, (y + 3) % 4, (y + 2) % 4
    zp, zm, z2 = (z + 1) % 4, (z + 3) % 4, (z + 2) % 4

    def at_x(k):
        return (((x + k) % 4) * 2 + c, local)

    def at_yz(a, b):
        return (node, a * 4 + b)

    mate = (x * 2 + 1 - c, local)
    xpd, xmd = at_x(1), at_x(3)
    ypd, ymd, zpd, zmd = at_yz(yp, z), at_yz(ym, z), at_yz(y, zp), at_yz(y, zm)
    d_z1, d_z3 = at_yz(y, z + 1 - 2 * (z % 2)), at_yz(y, 3 - z)
    d_y1, d_y3 = at_yz(y + 1 - 2 * (y % 2), z), at_yz(3 - y, z)

    def rc(src, dst, k, dev):
        return pltpu.make_async_remote_copy(
            src_ref=src, dst_ref=dst, send_sem=ssem.at[k], recv_sem=rsem.at[k],
            device_id=dev, device_id_type=MESH,
        )

    def go(copies):
        for cp in copies:
            cp.start()

    def done(copies):
        for cp in copies:
            cp.wait()

    def lane(q, base):
        return pl.ds(pl.multiple_of(base + 128 * q, 128), 128)

    left, right = pl.ds(0, TOK), pl.ds(TOK, TOK)
    ca = pl.ds(0, HALF)
    tok_rows, dy_rows, meta_rows = pl.ds(0, FEAT), pl.ds(FEAT, FEAT), pl.ds(2 * FEAT, 16)

    own = [
        pltpu.make_async_copy(routes_h, rbuf, lsem.at[0]),
        pltpu.make_async_copy(gates_h, gbuf, lsem.at[1]),
        pltpu.make_async_copy(tok_h, gat.at[0, tok_rows, left], lsem.at[2]),
        pltpu.make_async_copy(dy_h, gat.at[0, dy_rows, left], lsem.at[3]),
    ]
    go(own)
    weights = [pltpu.make_async_copy(h, wt.at[m], lsem.at[4 + m]) for m, h in enumerate((wg_h, wu_h, wd_h))]
    go(weights)
    barrier = pltpu.get_barrier_semaphore()
    for dev in (mate, xpd, xmd, ypd, ymd, zpd, zmd):
        pl.semaphore_signal(barrier, inc=1, device_id=dev, device_id_type=MESH)
    done(own[:2])
    gat[0, meta_rows, left] = jnp.concatenate([rbuf[...].astype(F32), gbuf[...].astype(F32)], 0).astype(BF)
    row_i = lax.broadcasted_iota(jnp.int32, (TOK, TOK), 0)
    col_i = lax.broadcasted_iota(jnp.int32, (TOK, TOK), 1)
    tri[...] = jnp.where(row_i < col_i, 1.0, 0.0).astype(BF)
    done(own[2:])
    pl.semaphore_wait(barrier, 7)
    first = [
        rc(gat.at[0, :, left], gat.at[0, :, right], 0, mate),
        rc(gat.at[0, :, left], gat.at[3, :, left], 1, xpd),
        rc(gat.at[0, :, left], gat.at[1, :, left], 2, xmd),
    ]
    second = [
        rc(gat.at[3, tok_rows, left], gat.at[2, tok_rows, left], 3, xpd),
        rc(gat.at[1, pl.ds(FEAT, BLK - FEAT), left], gat.at[2, pl.ds(FEAT, BLK - FEAT), left], 4, xmd),
        rc(gat.at[3, :, left], gat.at[3, :, right], 5, mate),
        rc(gat.at[1, :, left], gat.at[1, :, right], 6, mate),
    ]
    third = [rc(gat.at[2, :, left], gat.at[2, :, right], 7, mate)]
    go(first)

    def bufs(par):
        return (prt.at[par], r1a, r1b, r2a, r2b, sa, sb, r3a, r3b, r4a, r4b, act.at[par])

    half_bufs = (prt_h, r1a_h, r1b_h, r2a_h, r2b_h, sa_h, sb_h, r3a_h, r3b_h, r4a_h, r4b_h, act_h)
    k0 = Part(0, (0, CAPS), (0, TOK), CAPS, NLO, bufs(0), 20, 0, 0)
    k1 = Part(3, (0, ROWS), (0, PAIR), ROWS, CAPS, bufs(1), 20, 1, 1)
    k2 = Part(2, (0, ROWS), (0, PAIR), ROWS, CAPS, bufs(0), 20, 0, 0)
    k3 = Part(1, (0, ROWS), (0, PAIR), ROWS, CAPS, bufs(1), 20, 1, 1)
    kh = Part(0, (CAPS, ROWS), (TOK, PAIR), CAPS, NLO, half_bufs, 64, 0, 2)

    def meta_of(k):
        m = gat[k.r, meta_rows, k.ln].astype(F32)
        return m[:8], m[8:]

    def expert_id(e):
        return (node * EXP + e).astype(F32)

    def project(k):
        routes, _ = meta_of(k)
        wide = (16, k.width)
        rid = lax.broadcasted_iota(jnp.int32, wide, 0)
        member = jnp.zeros(wide, F32)
        for e in range(EXP):
            one = jnp.sum(jnp.where(routes == expert_id(e), 1.0, 0.0), axis=0, keepdims=True)
            member = jnp.where(rid == e, jnp.broadcast_to(one, wide), member)
        for h in range(k.width // TOK):
            mine = member[:, h * TOK : (h + 1) * TOK]
            before = dot_n(mine.astype(BF), tri[...])
            slot[:, pl.ds(h * TOK, TOK)] = jnp.where(mine > 0.5, before + float(CAPS * h), -1.0)
        sid = lax.broadcasted_iota(jnp.int32, (k.n, k.width), 0).astype(F32)

        def one_expert(e, carry):
            o = jnp.where(sid == slot[pl.ds(e, 1), pl.ds(0, k.width)], 1.0, 0.0).astype(BF)
            hot[k.r, e, k.rw, k.ln] = o
            xr = dot_t(o, gat[k.r, tok_rows, k.ln]).astype(BF)
            k.p[0, e, k.all] = dot_n(xr, wt[0, e]).astype(BF)
            k.p[1, e, k.all] = dot_n(xr, wt[1, e]).astype(BF)
            gr = dot_t(o, gat[k.r, dy_rows, k.ln]).astype(BF)
            k.p[2, e, k.all] = dot_n(gr, wt[2, e]).astype(BF)
            return carry

        lax.fori_loop(0, EXP, one_expert, 0)

    def s1(k):
        p, b = k.p, k.base
        return [
            rc(p.at[:, y2, k.lo, ca], k.r1a.at[0, :, k.nlo], b, ymd),
            rc(p.at[:, y2, k.hi, ca], k.r1a.at[1, :, k.nhi], b + 1, ypd),
            rc(p.at[:, :, k.lo, lane(z2, HALF)], k.r1b.at[0, :, :, k.nlo], b + 2, zmd),
            rc(p.at[:, :, k.hi, lane(z2, HALF)], k.r1b.at[1, :, :, k.nhi], b + 3, zpd),
        ]

    def s1_add(k):
        p = k.p
        for m in range(3):
            p[m, ym, k.lo, ca] = add2(p[m, ym, k.lo, ca], k.r1a[0, m, k.nlo])
            p[m, yp, k.hi, ca] = add2(p[m, yp, k.hi, ca], k.r1a[1, m, k.nhi])
            p[m, :, k.lo, lane(zm, HALF)] = add2(p[m, :, k.lo, lane(zm, HALF)], k.r1b[0, m, :, k.nlo])
            p[m, :, k.hi, lane(zp, HALF)] = add2(p[m, :, k.hi, lane(zp, HALF)], k.r1b[1, m, :, k.nhi])

    def s2(k):
        p, b = k.p, k.base + 4
        return [
            rc(p.at[:, yp, k.all, ca], k.r2a.at[0, :, k.all], b, ypd),
            rc(p.at[:, ym, k.all, ca], k.r2a.at[1, :, k.all], b + 1, ymd),
            rc(p.at[:, :, k.all, lane(zp, HALF)], k.r2b.at[0, :, :, k.all], b + 2, zpd),
            rc(p.at[:, :, k.all, lane(zm, HALF)], k.r2b.at[1, :, :, k.all], b + 3, zmd),
        ]

    def s2_add(k):
        p = k.p
        for m in range(3):
            k.sa[m, k.all] = add3(p[m, y, k.all, ca], k.r2a[0, m, k.all], k.r2a[1, m, k.all]).astype(BF)
            k.sb[m, :, k.all] = add3(
                p[m, :, k.all, lane(z, HALF)], k.r2b[0, m, :, k.all], k.r2b[1, m, :, k.all]
            ).astype(BF)

    def s3(k):
        b = k.base + 8
        return [
            rc(k.sa.at[:, k.lo, lane(z2, 0)], k.r3a.at[0, :, k.nlo], b, zmd),
            rc(k.sa.at[:, k.hi, lane(z2, 0)], k.r3a.at[1, :, k.nhi], b + 1, zpd),
            rc(k.sb.at[:, y2, k.lo], k.r3b.at[0, :, k.nlo], b + 2, ymd),
            rc(k.sb.at[:, y2, k.hi], k.r3b.at[1, :, k.nhi], b + 3, ypd),
        ]

    def s3_add(k):
        a, b = k.sa, k.sb
        for m in range(3):
            a[m, k.lo, lane(zm, 0)] = add2(a[m, k.lo, lane(zm, 0)], k.r3a[0, m, k.nlo])
            a[m, k.hi, lane(zp, 0)] = add2(a[m, k.hi, lane(zp, 0)], k.r3a[1, m, k.nhi])
            b[m, ym, k.lo] = add2(b[m, ym, k.lo], k.r3b[0, m, k.nlo])
            b[m, yp, k.hi] = add2(b[m, yp, k.hi], k.r3b[1, m, k.nhi])

    def s4(k):
        b = k.base + 12
        return [
            rc(k.sa.at[:, k.all, lane(zp, 0)], k.r4a.at[0, :, k.all], b, zpd),
            rc(k.sa.at[:, k.all, lane(zm, 0)], k.r4a.at[1, :, k.all], b + 1, zmd),
            rc(k.sb.at[:, yp, k.all], k.r4b.at[0, :, k.all], b + 2, ypd),
            rc(k.sb.at[:, ym, k.all], k.r4b.at[1, :, k.all], b + 3, ymd),
        ]

    def activate(k):
        routes, gates = meta_of(k)
        match = jnp.where(routes == expert_id(y), 1.0, 0.0)
        gate_row = jnp.sum(match * gates, axis=0, keepdims=True)
        oh = hot[k.r, y, k.rw, k.ln].astype(F32)
        q = jnp.sum(oh * gate_row, axis=1, keepdims=True)
        dots = jnp.zeros((k.n, 1), F32)
        for h in range(2):
            if h == 0:
                g, u, b = (
                    add3(k.sa[m, k.all, lane(z, 0)], k.r4a[0, m, k.all], k.r4a[1, m, k.all]) for m in range(3)
                )
            else:
                g, u, b = (add3(k.sb[m, y, k.all], k.r4b[0, m, k.all], k.r4b[1, m, k.all]) for m in range(3))
            logistic = 1.0 / (1.0 + jnp.exp(-g))
            swished = g * logistic
            hidden = swished * u
            dots = dots + jnp.sum(hidden * b, axis=1, keepdims=True)
            scaled = q * b
            at = lane(z, h * HALF)
            k.t[0, y, k.all, at] = (scaled * u * logistic * (1.0 + g * (1.0 - logistic))).astype(BF)
            k.t[1, y, k.all, at] = (scaled * swished).astype(BF)
            k.t[2, y, k.all, at] = (q * hidden).astype(BF)
        dv[k.d, 0, :, pl.ds(0, k.width)] = match * jnp.sum(oh * dots, axis=0, keepdims=True)

    def share(k, step, b, dev):
        at = pl.ds(0, k.width)
        return rc(dv.at[k.d, step, :, at], dr.at[k.d, step, :, at], b, dev)

    def a1(k):
        t, b = k.t, k.base + 16
        az, bz = t.at[:, y, k.all, lane(z, 0)], t.at[:, y, k.all, lane(z, HALF)]
        return [rc(az, az, b, zpd), rc(az, az, b + 1, zmd), rc(bz, bz, b + 2, ypd), rc(bz, bz, b + 3, ymd),
                share(k, 0, b + 4, d_z1)]

    def a2(k):
        t, b = k.t, k.base + 21
        v = [t.at[:, y, k.lo, lane(zm, 0)], t.at[:, y, k.hi, lane(zp, 0)],
             t.at[:, ym, k.lo, lane(z, HALF)], t.at[:, yp, k.hi, lane(z, HALF)]]
        return [rc(v[0], v[0], b, zpd), rc(v[1], v[1], b + 1, zmd), rc(v[2], v[2], b + 2, ypd),
                rc(v[3], v[3], b + 3, ymd), share(k, 1, b + 4, d_z3)]

    def a3(k):
        t, b = k.t, k.base + 26
        ay, bz = t.at[:, y, k.all, ca], t.at[:, :, k.all, lane(z, HALF)]
        return [rc(ay, ay, b, ypd), rc(ay, ay, b + 1, ymd), rc(bz, bz, b + 2, zpd), rc(bz, bz, b + 3, zmd),
                share(k, 2, b + 4, d_y1)]

    def a4(k):
        t, b = k.t, k.base + 31 + 5 * k.par
        v = [t.at[:, ym, k.lo, ca], t.at[:, yp, k.hi, ca],
             t.at[:, :, k.lo, lane(zm, HALF)], t.at[:, :, k.hi, lane(zp, HALF)]]
        return [rc(v[0], v[0], b, ypd), rc(v[1], v[1], b + 1, ymd), rc(v[2], v[2], b + 2, zpd),
                rc(v[3], v[3], b + 3, zmd), share(k, 3, b + 4, d_y3)]

    def dstep(k, step):
        at = pl.ds(0, k.width)
        dv[k.d, step + 1, :, at] = dv[k.d, step, :, at] + dr[k.d, step, :, at]

    def do_s1(k):
        done(s1(k))
        s1_add(k)
        go(s2(k))

    def do_s2(k):
        done(s2(k))
        s2_add(k)
        go(s3(k))

    def do_s3(k):
        done(s3(k))
        s3_add(k)
        go(s4(k))

    def do_a1(k):
        done(a1(k))
        dstep(k, 0)
        go(a2(k))

    def do_a2(k):
        done(a2(k))
        dstep(k, 1)
        go(a3(k))

    def do_a3(k):
        done(a3(k))
        dstep(k, 2)

    def post_a(k):
        done(a4(k))
        dstep(k, 3)
        at = pl.ds(0, k.width)
        bk[:, at] = jnp.zeros((FEAT, k.width), F32)

        def one_expert(e, carry):
            rb = dot_t(wt[0, e], k.t[0, e, k.all]) + dot_t(wt[1, e], k.t[1, e, k.all])
            bk[:, at] += dot_n(rb.astype(BF), hot[k.r, e, k.rw, k.ln])
            return carry

        lax.fori_loop(0, EXP, one_expert, 0)
        cb[k.r, tok_rows, k.ln] = bk[:, at].astype(BF)
        cb[k.r, pl.ds(FEAT, 16), k.ln] = jnp.concatenate(
            [dv[k.d, 4, :, at], jnp.zeros((8, k.width), F32)], 0
        ).astype(BF)

    def post_b(k, fresh=False):
        def one_expert(e, carry):
            xt = dot_t(gat[k.r, tok_rows, k.ln], hot[k.r, e, k.rw, k.ln]).astype(BF)
            gr = dot_t(gat[k.r, dy_rows, k.ln], hot[k.r, e, k.rw, k.ln]).astype(BF)
            for m, side in enumerate((xt, xt, gr)):
                new = dot_n(side, k.t[m, e, k.all])
                acc[m][e] = (new if fresh else acc[m][e].astype(F32) + new).astype(BF)
            return carry

        lax.fori_loop(0, EXP, one_expert, 0)

    def c1(r):
        return [rc(cb.at[r, :, right], c1r.at[r], 8 + r, mate)]

    def do_c1(r):
        done(c1(r))
        cs[r] = add2(cb[r, :, left], c1r[r])

    c2 = [rc(cs.at[2, pl.ds(0, CUT)], c2a, 12, xpd), rc(cs.at[2, pl.ds(CUT, CROWS - CUT)], c2b, 13, xmd)]
    c3 = [rc(cs.at[1], c3r.at[0], 14, xpd), rc(cs.at[3], c3r.at[1], 15, xmd)]

    done(weights)
    project(k0)
    go(s1(k0))
    done(first[:1])
    project(kh)
    go(s1(kh))
    do_s1(k0)
    do_s1(kh)
    done(first[1:])
    go(second)
    done(second[2:3])
    project(k1)
    do_s2(k0)
    go(s1(k1))
    do_s2(kh)
    do_s3(k0)
    do_s3(kh)
    done(s4(k0))
    activate(k0)
    go(a1(k0))
    do_s1(k1)
    done(s4(kh))
    activate(kh)
    do_a1(k0)
    done(second[:2])
    done(second[3:])
    go(third)
    do_a2(k0)

    done(third)
    project(k2)
    do_s2(k1)
    do_a3(k0)
    do_s3(k1)
    go(s1(k2))
    go(a4(k0))
    done(s4(k1))
    activate(k1)
    go(a1(k1))

    done(s1(k2))
    s1_add(k2)
    do_a1(k1)
    go(s2(k2))
    do_a2(k1)
    post_a(k0)
    post_b(k0, True)
    project(k3)
    do_s2(k2)
    do_a3(k1)
    do_s3(k2)
    go(s1(k3))
    go(a4(k1))
    done(s4(k2))
    activate(k2)
    go(a1(k2))

    done(s1(k3))
    s1_add(k3)
    do_a1(k2)
    go(s2(k3))
    do_a2(k2)
    post_a(k1)
    go(c1(3))
    post_b(k1)
    do_s2(k3)
    do_a3(k2)
    do_s3(k3)
    go(a4(k2))
    done(s4(k3))
    activate(k3)
    go(a1(k3))

    do_c1(3)
    do_a1(k3)
    do_a2(k3)
    go(a1(kh))
    post_a(k2)
    go(c1(2))
    post_b(k2)
    do_c1(2)
    go(c2)
    do_a3(k3)
    go(a4(k3))
    do_a1(kh)
    done(c2)
    cs[3, pl.ds(CUT, CROWS - CUT), :] = add2(cs[3, pl.ds(CUT, CROWS - CUT), :], c2b[...])
    c3[1].start()
    do_a2(kh)
    post_a(k3)
    go(c1(1))
    do_c1(1)
    cs[1, pl.ds(0, CUT), :] = add2(cs[1, pl.ds(0, CUT), :], c2a[...])
    c3[0].start()
    do_a3(kh)
    go(a4(kh))
    post_b(k3)
    post_a(kh)
    go(c1(0))
    post_b(kh)

    eid = lax.broadcasted_iota(jnp.int32, (1, ALL_EXPERTS), 1)
    ld[...] = jnp.zeros_like(ld)

    def one_block(b, carry):
        r = (b // 2 - x + 4) % 4
        cc = (b % 2 + c) % 2
        m = gat[r, meta_rows, pl.ds(pl.multiple_of(cc * TOK, TOK), TOK)].astype(F32)
        routes, gates = m[:8], m[8:]
        tot = jnp.zeros((1, ALL_EXPERTS), F32)
        for e in range(ALL_EXPERTS):
            s = jnp.sum(jnp.where(routes == float(e), gates, 0.0), axis=0, keepdims=True)
            s = jnp.sum(s, axis=1, keepdims=True)
            tot = jnp.where(eid == e, jnp.broadcast_to(s, (1, ALL_EXPERTS)), tot)
        ld[...] += tot
        return carry

    lax.fori_loop(0, 8, one_block, 0)
    ld[...] = ld[...] * (1.0 / 64.0)
    do_c1(0)
    done(c3)
    total = add3(cs[0], c3r[0], c3r[1])
    gt[...] = total[:FEAT].astype(BF)
    gg[...] = total[FEAT : FEAT + 8].astype(BF)


def on_device(tokens, grad_out, gates, routes, w_gate, w_up, w_down):
    any_ = pl.BlockSpec(memory_space=pl.ANY)
    V = pltpu.VMEM
    w_shape = (EXP, FEAT, HID)

    def comm(copies, rows, cut):
        lead = () if copies is None else (copies,)
        return [
            V((*lead, 3, EXP, rows, HID), BF),
            V((2, 3, cut, HALF), BF), V((2, 3, EXP, cut, 128), BF),
            V((2, 3, rows, HALF), BF), V((2, 3, EXP, rows, 128), BF),
            V((3, rows, HALF), BF), V((3, EXP, rows, 128), BF),
            V((2, 3, cut, 128), BF), V((2, 3, cut, 128), BF),
            V((2, 3, rows, 128), BF), V((2, 3, rows, 128), BF),
            V((*lead, 3, EXP, rows, HID), BF),
        ]

    scratch = [
        V((3, *w_shape), BF), V((4, BLK, PAIR), BF), V((TOK, TOK), BF), V((4, EXP, ROWS, PAIR), BF),
        V((16, PAIR), F32), V((8, TOK), jnp.int32), V((8, TOK), BF),
        *comm(2, ROWS, CAPS), *comm(None, CAPS, NLO),
        V((3, 5, 8, PAIR), F32), V((3, 4, 8, PAIR), F32), V((2, 8, PAIR), F32),
        V((FEAT, PAIR), F32), V((4, CROWS, PAIR), BF), V((4, CROWS, TOK), BF),
        V((4, CROWS, TOK), BF), V((CUT, TOK), BF), V((CROWS - CUT, TOK), BF), V((2, CROWS, TOK), BF),
        pltpu.SemaphoreType.DMA((7,)), pltpu.SemaphoreType.DMA((106,)), pltpu.SemaphoreType.DMA((106,)),
    ]
    gt, gg, ld, og, ou, od = pl.pallas_call(
        kernel,
        name="expert_backward",
        out_shape=(
            V((FEAT, TOK), BF), V((8, TOK), BF), V((1, ALL_EXPERTS), F32),
            V(w_shape, BF), V(w_shape, BF), V(w_shape, BF),
        ),
        in_specs=[any_] * 7,
        out_specs=[pl.BlockSpec(memory_space=pltpu.VMEM)] * 6,
        scratch_shapes=scratch,
        compiler_params=pltpu.CompilerParams(
            collective_id=0, has_side_effects=True, vmem_limit_bytes=54_500_000
        ),
    )(routes.T, gates.T, tokens.T, grad_out.T, w_gate, w_up, jnp.transpose(w_down, (0, 2, 1)))
    return gt.T, gg.T, og, ou, jnp.transpose(od, (0, 2, 1)), ld.reshape(ALL_EXPERTS)


def solution(mesh):
    in_specs = (
        P("node", "local"),
        P("node", "local"),
        P("node", None),
        P("node", None),
        P("node", "local", None),
        P("node", "local", None),
        P("node", None, "local"),
    )
    out_specs = (
        P("node", "local"),
        P("node", None),
        P("node", "local", None),
        P("node", "local", None),
        P("node", None, "local"),
        P(),
    )
    return jax.shard_map(
        on_device, mesh=mesh, in_specs=in_specs, out_specs=out_specs, check_vma=False
    )
```

```python
import jax
import jax.numpy as jnp
from jax import lax
from jax.experimental import pallas as pl
from jax.experimental.pallas import tpu as pltpu
from jax.sharding import PartitionSpec as P

BF = jnp.bfloat16
F32 = jnp.float32
MESH = pl.DeviceIdType.MESH
FEAT, TOK, HID, CAPS, EXP = 448, 256, 1024, 80, 4
PAIR = 2 * TOK
ROWS = 2 * CAPS
NLO = 48
HALF = HID // 2
BLK = 2 * FEAT + 16
CROWS = FEAT + 16
CUT = 224
ALL_EXPERTS = 32


def dot_t(a, b):
    return lax.dot_general(a, b, (((1,), (1,)), ((), ())), preferred_element_type=F32)


def dot_n(a, b):
    return jnp.dot(a, b, preferred_element_type=F32)


def add2(a, b):
    return (a.astype(F32) + b.astype(F32)).astype(BF)


def add3(a, b, c):
    return a.astype(F32) + b.astype(F32) + c.astype(F32)


class Part:
    def __init__(self, r, rows, lanes, local_rows, cut, bufs, base, par, dpar):
        self.r, self.rows, self.lanes, self.n, self.cut = r, rows, lanes, local_rows, cut
        self.width = lanes[1] - lanes[0]
        (self.p, self.r1a, self.r1b, self.r2a, self.r2b, self.sa, self.sb,
         self.r3a, self.r3b, self.r4a, self.r4b, self.t) = bufs
        self.base, self.par, self.d = base, par, dpar
        self.lo, self.hi = pl.ds(0, cut), pl.ds(cut, local_rows - cut)
        self.nlo, self.nhi = pl.ds(0, cut), pl.ds(0, local_rows - cut)
        self.all = pl.ds(0, local_rows)
        self.ln = pl.ds(lanes[0], self.width)
        self.rw = pl.ds(rows[0], local_rows)


def kernel(
    routes_h, gates_h, tok_h, dy_h, wg_h, wu_h, wd_h,
    gt, gg, ld, acc0, acc1, acc2,
    wt, gat, tri, hot, slot, xb, rbuf, gbuf, prt, r1a, r1b, r2a, r2b, sa, sb, r3a, r3b, r4a, r4b, act,
    prt_h, r1a_h, r1b_h, r2a_h, r2b_h, sa_h, sb_h, r3a_h, r3b_h, r4a_h, r4b_h, act_h,
    dv, dr, df, bk, cb, c1r, cs, c2a, c2b, c3r,
    lsem, ssem, rsem,
):
    acc = (acc0, acc1, acc2)
    node, local = lax.axis_index("node"), lax.axis_index("local")
    x, c = node // 2, node % 2
    y, z = local // 4, local % 4
    yp, ym, y2 = (y + 1) % 4, (y + 3) % 4, (y + 2) % 4
    zp, zm, z2 = (z + 1) % 4, (z + 3) % 4, (z + 2) % 4

    def at_x(k):
        return (((x + k) % 4) * 2 + c, local)

    def at_yz(a, b):
        return (node, a * 4 + b)

    mate = (x * 2 + 1 - c, local)
    xpd, xmd = at_x(1), at_x(3)
    ypd, ymd, zpd, zmd = at_yz(yp, z), at_yz(ym, z), at_yz(y, zp), at_yz(y, zm)
    d_z1, d_z3 = at_yz(y, z + 1 - 2 * (z % 2)), at_yz(y, 3 - z)
    d_y1, d_y3 = at_yz(y + 1 - 2 * (y % 2), z), at_yz(3 - y, z)

    def rc(src, dst, k, dev):
        return pltpu.make_async_remote_copy(
            src_ref=src, dst_ref=dst, send_sem=ssem.at[k], recv_sem=rsem.at[k],
            device_id=dev, device_id_type=MESH,
        )

    def go(copies):
        for cp in copies:
            cp.start()

    def done(copies):
        for cp in copies:
            cp.wait()

    def lane(q, base):
        return pl.ds(pl.multiple_of(base + 128 * q, 128), 128)

    left, right = pl.ds(0, TOK), pl.ds(TOK, TOK)
    ca = pl.ds(0, HALF)
    tok_rows, dy_rows, meta_rows = pl.ds(0, FEAT), pl.ds(FEAT, FEAT), pl.ds(2 * FEAT, 16)

    own = [
        pltpu.make_async_copy(routes_h, rbuf, lsem.at[0]),
        pltpu.make_async_copy(gates_h, gbuf, lsem.at[1]),
        pltpu.make_async_copy(tok_h, gat.at[0, tok_rows, left], lsem.at[2]),
        pltpu.make_async_copy(dy_h, gat.at[0, dy_rows, left], lsem.at[3]),
    ]
    go(own)
    weights = [pltpu.make_async_copy(h, wt.at[m], lsem.at[4 + m]) for m, h in enumerate((wg_h, wu_h, wd_h))]
    go(weights[:1])
    barrier = pltpu.get_barrier_semaphore()
    for dev in (mate, xpd, xmd, ypd, ymd, zpd, zmd):
        pl.semaphore_signal(barrier, inc=1, device_id=dev, device_id_type=MESH)
    done(own[:2])
    gat[0, meta_rows, left] = jnp.concatenate([rbuf[...].astype(F32), gbuf[...].astype(F32)], 0).astype(BF)
    row_i = lax.broadcasted_iota(jnp.int32, (TOK, TOK), 0)
    col_i = lax.broadcasted_iota(jnp.int32, (TOK, TOK), 1)
    tri[...] = jnp.where(row_i < col_i, 1.0, 0.0).astype(BF)
    done(own[2:])
    go(weights[1:])
    pl.semaphore_wait(barrier, 7)
    first = [
        rc(gat.at[0, :, left], gat.at[0, :, right], 0, mate),
        rc(gat.at[0, :, left], gat.at[3, :, left], 1, xpd),
        rc(gat.at[0, :, left], gat.at[1, :, left], 2, xmd),
    ]
    second = [
        rc(gat.at[3, tok_rows, left], gat.at[2, tok_rows, left], 3, xpd),
        rc(gat.at[1, pl.ds(FEAT, BLK - FEAT), left], gat.at[2, pl.ds(FEAT, BLK - FEAT), left], 4, xmd),
        rc(gat.at[3, :, left], gat.at[3, :, right], 5, mate),
        rc(gat.at[1, :, left], gat.at[1, :, right], 6, mate),
    ]
    third = [rc(gat.at[2, :, left], gat.at[2, :, right], 7, mate)]
    go(first)

    def bufs(par):
        return (prt.at[par], r1a, r1b, r2a, r2b, sa, sb, r3a, r3b, r4a, r4b, act.at[par])

    half_bufs = (prt_h, r1a_h, r1b_h, r2a_h, r2b_h, sa_h, sb_h, r3a_h, r3b_h, r4a_h, r4b_h, act_h)
    k0 = Part(0, (0, CAPS), (0, TOK), CAPS, NLO, bufs(0), 20, 0, 0)
    k1 = Part(3, (0, ROWS), (0, PAIR), ROWS, CAPS, bufs(1), 20, 1, 1)
    k2 = Part(2, (0, ROWS), (0, PAIR), ROWS, CAPS, bufs(0), 20, 0, 0)
    k3 = Part(1, (0, ROWS), (0, PAIR), ROWS, CAPS, bufs(1), 20, 1, 1)
    kh = Part(0, (CAPS, ROWS), (TOK, PAIR), CAPS, NLO, half_bufs, 80, 0, 2)

    def meta_of(k):
        m = gat[k.r, meta_rows, k.ln].astype(F32)
        return m[:8], m[8:]

    def expert_id(e):
        return (node * EXP + e).astype(F32)

    def project(k, load=False):
        routes, _ = meta_of(k)
        wide = (16, k.width)
        rid = lax.broadcasted_iota(jnp.int32, wide, 0)
        member = jnp.zeros(wide, F32)
        for e in range(EXP):
            one = jnp.sum(jnp.where(routes == expert_id(e), 1.0, 0.0), axis=0, keepdims=True)
            member = jnp.where(rid == e, jnp.broadcast_to(one, wide), member)
        for h in range(k.width // TOK):
            mine = member[:, h * TOK : (h + 1) * TOK]
            before = dot_n(mine.astype(BF), tri[...])
            slot[:, pl.ds(h * TOK, TOK)] = jnp.where(mine > 0.5, before + float(CAPS * h), -1.0)
        sid = lax.broadcasted_iota(jnp.int32, (k.n, k.width), 0).astype(F32)

        def rows_of(e, carry):
            o = jnp.where(sid == slot[pl.ds(e, 1), pl.ds(0, k.width)], 1.0, 0.0).astype(BF)
            hot[k.r, e, k.rw, k.ln] = o
            xb[0, e, k.all] = dot_t(o, gat[k.r, tok_rows, k.ln]).astype(BF)
            xb[1, e, k.all] = dot_t(o, gat[k.r, dy_rows, k.ln]).astype(BF)
            return carry

        lax.fori_loop(0, EXP, rows_of, 0)

        if load:
            for m in range(3):
                done(weights[m : m + 1])

                def one_product(e, carry):
                    k.p[m, e, k.all] = dot_n(xb[m // 2, e, k.all], wt[m, e]).astype(BF)
                    return carry

                lax.fori_loop(0, EXP, one_product, 0)
        else:

            def products(e, carry):
                for m in range(3):
                    k.p[m, e, k.all] = dot_n(xb[m // 2, e, k.all], wt[m, e]).astype(BF)
                return carry

            lax.fori_loop(0, EXP, products, 0)

    def s1(k):
        p, b = k.p, k.base
        return [
            rc(p.at[:, y2, k.lo, ca], k.r1a.at[0, :, k.nlo], b, ymd),
            rc(p.at[:, y2, k.hi, ca], k.r1a.at[1, :, k.nhi], b + 1, ypd),
            rc(p.at[:, :, k.lo, lane(z2, HALF)], k.r1b.at[0, :, :, k.nlo], b + 2, zmd),
            rc(p.at[:, :, k.hi, lane(z2, HALF)], k.r1b.at[1, :, :, k.nhi], b + 3, zpd),
        ]

    def s1_add(k):
        p = k.p
        for m in range(3):
            p[m, ym, k.lo, ca] = add2(p[m, ym, k.lo, ca], k.r1a[0, m, k.nlo])
            p[m, yp, k.hi, ca] = add2(p[m, yp, k.hi, ca], k.r1a[1, m, k.nhi])
            p[m, :, k.lo, lane(zm, HALF)] = add2(p[m, :, k.lo, lane(zm, HALF)], k.r1b[0, m, :, k.nlo])
            p[m, :, k.hi, lane(zp, HALF)] = add2(p[m, :, k.hi, lane(zp, HALF)], k.r1b[1, m, :, k.nhi])

    def s2(k, g):
        p, b, ms = k.p, k.base + 4 + 4 * g, (pl.ds(0, 1), pl.ds(1, 2))[g]
        return [
            rc(p.at[ms, yp, k.all, ca], k.r2a.at[0, ms, k.all], b, ypd),
            rc(p.at[ms, ym, k.all, ca], k.r2a.at[1, ms, k.all], b + 1, ymd),
            rc(p.at[ms, :, k.all, lane(zp, HALF)], k.r2b.at[0, ms, :, k.all], b + 2, zpd),
            rc(p.at[ms, :, k.all, lane(zm, HALF)], k.r2b.at[1, ms, :, k.all], b + 3, zmd),
        ]

    def s2_add(k):
        p = k.p
        for m in range(3):
            k.sa[m, k.all] = add3(p[m, y, k.all, ca], k.r2a[0, m, k.all], k.r2a[1, m, k.all]).astype(BF)
            k.sb[m, :, k.all] = add3(
                p[m, :, k.all, lane(z, HALF)], k.r2b[0, m, :, k.all], k.r2b[1, m, :, k.all]
            ).astype(BF)

    def s3(k):
        b = k.base + 12
        return [
            rc(k.sa.at[:, k.lo, lane(z2, 0)], k.r3a.at[0, :, k.nlo], b, zmd),
            rc(k.sa.at[:, k.hi, lane(z2, 0)], k.r3a.at[1, :, k.nhi], b + 1, zpd),
            rc(k.sb.at[:, y2, k.lo], k.r3b.at[0, :, k.nlo], b + 2, ymd),
            rc(k.sb.at[:, y2, k.hi], k.r3b.at[1, :, k.nhi], b + 3, ypd),
        ]

    def s3_add(k):
        a, b = k.sa, k.sb
        for m in range(3):
            a[m, k.lo, lane(zm, 0)] = add2(a[m, k.lo, lane(zm, 0)], k.r3a[0, m, k.nlo])
            a[m, k.hi, lane(zp, 0)] = add2(a[m, k.hi, lane(zp, 0)], k.r3a[1, m, k.nhi])
            b[m, ym, k.lo] = add2(b[m, ym, k.lo], k.r3b[0, m, k.nlo])
            b[m, yp, k.hi] = add2(b[m, yp, k.hi], k.r3b[1, m, k.nhi])

    def s4(k):
        b = k.base + 16
        return [
            rc(k.sa.at[:, k.all, lane(zp, 0)], k.r4a.at[0, :, k.all], b, zpd),
            rc(k.sa.at[:, k.all, lane(zm, 0)], k.r4a.at[1, :, k.all], b + 1, zmd),
            rc(k.sb.at[:, yp, k.all], k.r4b.at[0, :, k.all], b + 2, ypd),
            rc(k.sb.at[:, ym, k.all], k.r4b.at[1, :, k.all], b + 3, ymd),
        ]

    def activate(k):
        routes, gates = meta_of(k)
        match = jnp.where(routes == expert_id(y), 1.0, 0.0)
        gate_row = jnp.sum(match * gates, axis=0, keepdims=True)
        oh = hot[k.r, y, k.rw, k.ln].astype(F32)
        q = jnp.sum(oh * gate_row, axis=1, keepdims=True)
        dots = jnp.zeros((k.n, 1), F32)
        for h in range(2):
            if h == 0:
                g, u, b = (
                    add3(k.sa[m, k.all, lane(z, 0)], k.r4a[0, m, k.all], k.r4a[1, m, k.all]) for m in range(3)
                )
            else:
                g, u, b = (add3(k.sb[m, y, k.all], k.r4b[0, m, k.all], k.r4b[1, m, k.all]) for m in range(3))
            logistic = 1.0 / (1.0 + jnp.exp(-g))
            swished = g * logistic
            hidden = swished * u
            dots = dots + jnp.sum(hidden * b, axis=1, keepdims=True)
            scaled = q * b
            at = lane(z, h * HALF)
            k.t[0, y, k.all, at] = (scaled * u * logistic * (1.0 + g * (1.0 - logistic))).astype(BF)
            k.t[1, y, k.all, at] = (scaled * swished).astype(BF)
            k.t[2, y, k.all, at] = (q * hidden).astype(BF)
        dv[k.d, 0, :, pl.ds(0, k.width)] = match * jnp.sum(oh * dots, axis=0, keepdims=True)

    def share(k, step, b, dev):
        at = pl.ds(0, k.width)
        return rc(dv.at[k.d, step, :, at], dr.at[k.d, step, :, at], b, dev)

    def a1(k):
        t, b = k.t, k.base + 20
        az, bz = t.at[:, y, k.all, lane(z, 0)], t.at[:, y, k.all, lane(z, HALF)]
        return [rc(az, az, b, zpd), rc(az, az, b + 1, zmd), rc(bz, bz, b + 2, ypd), rc(bz, bz, b + 3, ymd),
                share(k, 0, b + 4, d_z1)]

    def a2(k):
        t, b = k.t, k.base + 25
        v = [t.at[:, y, k.lo, lane(zm, 0)], t.at[:, y, k.hi, lane(zp, 0)],
             t.at[:, ym, k.lo, lane(z, HALF)], t.at[:, yp, k.hi, lane(z, HALF)]]
        return [rc(v[0], v[0], b, zpd), rc(v[1], v[1], b + 1, zmd), rc(v[2], v[2], b + 2, ypd),
                rc(v[3], v[3], b + 3, ymd), share(k, 1, b + 4, d_z3)]

    def a3(k, g):
        t, b, ms = k.t, k.base + 30 + 4 * g, (pl.ds(0, 2), pl.ds(2, 1))[g]
        ay, bz = t.at[ms, y, k.all, ca], t.at[ms, :, k.all, lane(z, HALF)]
        own_share = [share(k, 2, b + 4, d_y1)] if g else []
        return [rc(ay, ay, b, ypd), rc(ay, ay, b + 1, ymd), rc(bz, bz, b + 2, zpd), rc(bz, bz, b + 3, zmd),
                *own_share]

    def a4(k, g):
        t, b, ms = k.t, k.base + 39 + 9 * k.par + 4 * g, (pl.ds(0, 2), pl.ds(2, 1))[g]
        v = [t.at[ms, ym, k.lo, ca], t.at[ms, yp, k.hi, ca],
             t.at[ms, :, k.lo, lane(zm, HALF)], t.at[ms, :, k.hi, lane(zp, HALF)]]
        own_share = [share(k, 3, b + 4, d_y3)] if g else []
        return [rc(v[0], v[0], b, ypd), rc(v[1], v[1], b + 1, ymd), rc(v[2], v[2], b + 2, zpd),
                rc(v[3], v[3], b + 3, zmd), *own_share]

    def dstep(k, step):
        at = pl.ds(0, k.width)
        dv[k.d, step + 1, :, at] = dv[k.d, step, :, at] + dr[k.d, step, :, at]

    def do_s1(k):
        done(s1(k))
        s1_add(k)
        go(s2(k, 0))
        go(s2(k, 1))

    def do_s2(k):
        done(s2(k, 0))
        done(s2(k, 1))
        s2_add(k)
        go(s3(k))

    def do_s3(k):
        done(s3(k))
        s3_add(k)
        go(s4(k))

    def do_a1(k):
        done(a1(k))
        dstep(k, 0)
        go(a2(k))

    def do_a2(k):
        done(a2(k))
        dstep(k, 1)
        go(a3(k, 0))

    def do_a3(k):
        done(a3(k, 0))
        done(a3(k, 1))
        dstep(k, 2)

    def arrive(k):
        done(a4(k, 0))
        done(a4(k, 1))
        dstep(k, 3)

    def post_a(k, start=0, size=FEAT, between=None):
        at, fr = pl.ds(0, k.width), pl.ds(start, size)
        bk[fr, at] = jnp.zeros((size, k.width), F32)

        def one_expert(e, carry):
            rb = dot_t(wt[0, e, fr], k.t[0, e, k.all]) + dot_t(wt[1, e, fr], k.t[1, e, k.all])
            bk[fr, at] += dot_n(rb.astype(BF), hot[k.r, e, k.rw, k.ln])
            return carry

        if between is None:
            lax.fori_loop(0, EXP, one_expert, 0)
        else:
            lax.fori_loop(0, EXP // 2, one_expert, 0)
            between()
            lax.fori_loop(EXP // 2, EXP, one_expert, 0)
        cb[k.r, fr, k.ln] = bk[fr, at].astype(BF)
        if start + size == FEAT:
            cb[k.r, pl.ds(FEAT, 16), k.ln] = jnp.concatenate(
                [dv[k.d, 4, :, at], jnp.zeros((8, k.width), F32)], 0
            ).astype(BF)

    def post_b(k, fresh=False):
        def one_expert(e, carry):
            xt = dot_t(gat[k.r, tok_rows, k.ln], hot[k.r, e, k.rw, k.ln]).astype(BF)
            gr = dot_t(gat[k.r, dy_rows, k.ln], hot[k.r, e, k.rw, k.ln]).astype(BF)
            for m, side in enumerate((xt, xt, gr)):
                new = dot_n(side, k.t[m, e, k.all])
                acc[m][e] = (new if fresh else acc[m][e].astype(F32) + new).astype(BF)
            return carry

        lax.fori_loop(0, EXP, one_expert, 0)

    def c1(r):
        return [rc(cb.at[r, :, right], c1r.at[r], 8 + r, mate)]

    def do_c1(r):
        done(c1(r))
        cs[r] = add2(cb[r, :, left], c1r[r])

    top, low = pl.ds(0, CUT), pl.ds(CUT, CROWS - CUT)
    c2 = [rc(cs.at[2, top], c2a, 12, xpd), rc(cs.at[2, low], c2b, 13, xmd)]
    c1_last = [rc(cb.at[1, top, right], c1r.at[1, top], 9, mate), rc(cb.at[1, low, right], c1r.at[1, low], 16, mate)]
    c3 = [
        rc(cs.at[1, top], c3r.at[0, top], 14, xpd),
        rc(cs.at[1, low], c3r.at[0, low], 17, xpd),
        rc(cs.at[3], c3r.at[1], 15, xmd),
    ]

    def count_loads():
        eid = lax.broadcasted_iota(jnp.int32, (1, ALL_EXPERTS), 1)
        ld[...] = jnp.zeros_like(ld)

        def one_block(b, carry):
            r = (b // 2 - x + 4) % 4
            cc = (b % 2 + c) % 2
            m = gat[r, meta_rows, pl.ds(pl.multiple_of(cc * TOK, TOK), TOK)].astype(F32)
            routes, gates = m[:8], m[8:]
            tot = jnp.zeros((1, ALL_EXPERTS), F32)
            for e in range(ALL_EXPERTS):
                v = jnp.sum(jnp.where(routes == float(e), gates, 0.0), axis=0, keepdims=True)
                v = jnp.sum(v, axis=1, keepdims=True)
                tot = jnp.where(eid == e, jnp.broadcast_to(v, (1, ALL_EXPERTS)), tot)
            ld[...] += tot
            return carry

        lax.fori_loop(0, 8, one_block, 0)
        ld[...] = ld[...] * (1.0 / 64.0)

    project(k0, True)
    go(s1(k0))
    done(first[:1])
    project(kh)
    go(s1(kh))
    do_s1(k0)
    do_s1(kh)
    done(first[1:])
    go(second)
    done(second[2:3])
    project(k1)
    do_s2(k0)
    go(s1(k1))
    do_s2(kh)
    do_s3(k0)
    done(second[:2])
    done(second[3:])
    go(third)
    done(s1(k1))
    s1_add(k1)
    go(s2(k1, 0))
    done(s4(k0))
    activate(k0)
    go(a1(k0))
    do_s3(kh)
    go(s2(k1, 1))

    done(third)
    count_loads()
    project(k2)
    do_a1(k0)
    done(s4(kh))
    activate(kh)
    go(a1(kh))
    do_s2(k1)
    do_a2(k0)
    go(a3(k0, 1))
    do_s3(k1)
    go(s1(k2))
    done(s4(k1))
    activate(k1)
    go(a1(k1))

    done(s1(k2))
    s1_add(k2)
    go(s2(k2, 0))
    do_a3(k0)
    go(a4(k0, 0))
    go(a4(k0, 1))
    do_a1(k1)
    go(s2(k2, 1))
    do_a2(k1)
    arrive(k0)
    post_a(k0)
    post_b(k0, True)
    do_s2(k2)
    go(a3(k1, 1))
    project(k3)
    do_s3(k2)
    go(s1(k3))
    do_a3(k1)
    go(a4(k1, 0))
    go(a4(k1, 1))
    do_a1(kh)
    done(s4(k2))
    activate(k2)
    go(a1(k2))

    done(s1(k3))
    s1_add(k3)
    go(s2(k3, 0))
    do_a1(k2)
    go(s2(k3, 1))
    do_a2(k2)
    arrive(k1)
    post_a(k1)
    go(c1(3))
    post_b(k1)
    do_s2(k3)
    go(a3(k2, 1))
    do_s3(k3)
    do_a3(k2)
    go(a4(k2, 0))
    go(a4(k2, 1))
    done(s4(k3))
    activate(k3)
    go(a1(k3))

    do_a2(kh)
    go(a3(kh, 1))
    do_c1(3)
    do_a1(k3)
    do_a3(kh)
    go(a4(kh, 0))
    go(a4(kh, 1))
    do_a2(k3)
    go(a3(k3, 1))
    arrive(k2)
    post_a(k2)
    go(c1(2))
    post_b(k2)
    do_c1(2)
    go(c2)
    done(a3(k3, 0))
    go(a4(k3, 0))
    arrive(kh)
    post_a(kh)
    go(c1(0))
    done(a3(k3, 1))
    dstep(k3, 2)
    go(a4(k3, 1))
    done(c2)
    cs[3, low, :] = add2(cs[3, low, :], c2b[...])
    c3[2].start()
    post_b(kh)
    do_c1(0)
    done(a4(k3, 0))
    post_a(k3, 0, CUT)
    c1_last[0].start()
    done(a4(k3, 1))
    dstep(k3, 3)

    def send_top():
        c1_last[0].wait()
        cs[1, top, :] = add3(cb[1, top, left], c1r[1, top], c2a[...]).astype(BF)
        c3[0].start()

    post_a(k3, CUT, FEAT - CUT, send_top)
    c1_last[1].start()
    c1_last[1].wait()
    cs[1, low, :] = add2(cb[1, low, left], c1r[1, low])
    c3[1].start()
    post_b(k3)
    c3[2].wait()
    c3[0].wait()
    gt[top, :] = add3(cs[0, top], c3r[0, top], c3r[1, top]).astype(BF)
    c3[1].wait()
    rest = add3(cs[0, low], c3r[0, low], c3r[1, low])
    gt[pl.ds(CUT, FEAT - CUT), :] = rest[: FEAT - CUT].astype(BF)
    gg[...] = rest[FEAT - CUT : FEAT - CUT + 8].astype(BF)


def flush(g0, g1, g2, g3, g4, g5, o0, o1, o2, o3, o4, o5, sem):
    copies = [
        pltpu.make_async_copy(a, b, sem.at[n])
        for n, (a, b) in enumerate(((g3, o3), (g4, o4), (g5, o5), (g0, o0), (g1, o1), (g2, o2)))
    ]
    for cp in copies:
        cp.start()
    for cp in copies:
        cp.wait()


def on_device(tokens, grad_out, gates, routes, w_gate, w_up, w_down):
    any_ = pl.BlockSpec(memory_space=pl.ANY)
    V = pltpu.VMEM
    w_shape = (EXP, FEAT, HID)

    def comm(copies, rows, cut):
        lead = () if copies is None else (copies,)
        return [
            V((*lead, 3, EXP, rows, HID), BF),
            V((2, 3, cut, HALF), BF), V((2, 3, EXP, cut, 128), BF),
            V((2, 3, rows, HALF), BF), V((2, 3, EXP, rows, 128), BF),
            V((3, rows, HALF), BF), V((3, EXP, rows, 128), BF),
            V((2, 3, cut, 128), BF), V((2, 3, cut, 128), BF),
            V((2, 3, rows, 128), BF), V((2, 3, rows, 128), BF),
            V((*lead, 3, EXP, rows, HID), BF),
        ]

    scratch = [
        V((3, *w_shape), BF), V((4, BLK, PAIR), BF), V((TOK, TOK), BF), V((4, EXP, ROWS, PAIR), BF),
        V((16, PAIR), F32), V((2, EXP, ROWS, FEAT), BF), V((8, TOK), jnp.int32), V((8, TOK), BF),
        *comm(2, ROWS, CAPS), *comm(None, CAPS, NLO),
        V((3, 5, 8, PAIR), F32), V((3, 4, 8, PAIR), F32), V((2, 8, PAIR), F32),
        V((FEAT, PAIR), F32), V((4, CROWS, PAIR), BF), V((4, CROWS, TOK), BF),
        V((4, CROWS, TOK), BF), V((CUT, TOK), BF), V((CROWS - CUT, TOK), BF), V((2, CROWS, TOK), BF),
        pltpu.SemaphoreType.DMA((7,)), pltpu.SemaphoreType.DMA((128,)), pltpu.SemaphoreType.DMA((128,)),
    ]
    results = pl.pallas_call(
        kernel,
        name="expert_backward",
        out_shape=(
            V((FEAT, TOK), BF), V((8, TOK), BF), V((1, ALL_EXPERTS), F32),
            V(w_shape, BF), V(w_shape, BF), V(w_shape, BF),
        ),
        in_specs=[any_] * 7,
        out_specs=[pl.BlockSpec(memory_space=pltpu.VMEM)] * 6,
        scratch_shapes=scratch,
        compiler_params=pltpu.CompilerParams(
            collective_id=0, has_side_effects=True, vmem_limit_bytes=54_000_000
        ),
    )(routes.T, gates.T, tokens.T, grad_out.T, w_gate, w_up, jnp.transpose(w_down, (0, 2, 1)))
    shape = jax.ShapeDtypeStruct
    gt, gg, ld, og, ou, od = pl.pallas_call(
        flush,
        name="write_results",
        out_shape=(
            shape((FEAT, TOK), BF), shape((8, TOK), BF), shape((1, ALL_EXPERTS), F32),
            shape(w_shape, BF), shape(w_shape, BF), shape(w_shape, BF),
        ),
        in_specs=[pl.BlockSpec(memory_space=pltpu.VMEM)] * 6,
        out_specs=[any_] * 6,
        scratch_shapes=[pltpu.SemaphoreType.DMA((6,))],
        compiler_params=pltpu.CompilerParams(vmem_limit_bytes=8_000_000),
    )(*results)
    return gt.T, gg.T, og, ou, jnp.transpose(od, (0, 2, 1)), ld.reshape(ALL_EXPERTS)


def solution(mesh):
    in_specs = (
        P("node", "local"),
        P("node", "local"),
        P("node", None),
        P("node", None),
        P("node", "local", None),
        P("node", "local", None),
        P("node", None, "local"),
    )
    out_specs = (
        P("node", "local"),
        P("node", None),
        P("node", "local", None),
        P("node", "local", None),
        P("node", None, "local"),
        P(),
    )
    return jax.shard_map(
        on_device, mesh=mesh, in_specs=in_specs, out_specs=out_specs, check_vma=False
    )
```

```python
import jax
import jax.numpy as jnp
from jax import lax
from jax.experimental import pallas as pl
from jax.experimental.pallas import tpu as pltpu
from jax.sharding import PartitionSpec as P

BF = jnp.bfloat16
F32 = jnp.float32
MESH = pl.DeviceIdType.MESH
FEAT, TOK, HID, CAPS, EXP = 448, 256, 1024, 80, 4
PAIR = 2 * TOK
ROWS = 2 * CAPS
NLO = 48
HALF = HID // 2
BLK = 2 * FEAT + 16
CROWS = FEAT + 16
CUT = 224
ALL_EXPERTS = 32


def dot_t(a, b):
    return lax.dot_general(a, b, (((1,), (1,)), ((), ())), preferred_element_type=F32)


def dot_n(a, b):
    return jnp.dot(a, b, preferred_element_type=F32)


def add2(a, b):
    return (a.astype(F32) + b.astype(F32)).astype(BF)


def add3(a, b, c):
    return a.astype(F32) + b.astype(F32) + c.astype(F32)


class Part:
    def __init__(self, r, rows, lanes, local_rows, cut, bufs, base, par, dpar):
        self.r, self.rows, self.lanes, self.n, self.cut = r, rows, lanes, local_rows, cut
        self.width = lanes[1] - lanes[0]
        (self.p, self.r1a, self.r1b, self.r2a, self.r2b, self.sa, self.sb,
         self.r3a, self.r3b, self.r4a, self.r4b, self.t) = bufs
        self.base, self.par, self.d = base, par, dpar
        self.lo, self.hi = pl.ds(0, cut), pl.ds(cut, local_rows - cut)
        self.nlo, self.nhi = pl.ds(0, cut), pl.ds(0, local_rows - cut)
        self.all = pl.ds(0, local_rows)
        self.ln = pl.ds(lanes[0], self.width)
        self.rw = pl.ds(rows[0], local_rows)


def kernel(
    routes_h, gates_h, tok_h, dy_h, wg_h, wu_h, wd_h,
    gt, gg, ld, acc0, acc1, acc2,
    wt, gat, tri, hot, slot, xb, tb, rbuf, gbuf, prt, r1a, r1b, r2a, r2b, sa, sb, r3a, r3b, r4a, r4b, act,
    prt_h, r1a_h, r1b_h, r2a_h, r2b_h, sa_h, sb_h, r3a_h, r3b_h, r4a_h, r4b_h, act_h,
    dv, dr, df, bk, cb, c1r, cs, c2a, c2b, c3r,
    lsem, ssem, rsem,
):
    acc = (acc0, acc1, acc2)
    node, local = lax.axis_index("node"), lax.axis_index("local")
    x, c = node // 2, node % 2
    y, z = local // 4, local % 4
    yp, ym, y2 = (y + 1) % 4, (y + 3) % 4, (y + 2) % 4
    zp, zm, z2 = (z + 1) % 4, (z + 3) % 4, (z + 2) % 4

    def at_x(k):
        return (((x + k) % 4) * 2 + c, local)

    def at_yz(a, b):
        return (node, a * 4 + b)

    mate = (x * 2 + 1 - c, local)
    xpd, xmd = at_x(1), at_x(3)
    ypd, ymd, zpd, zmd = at_yz(yp, z), at_yz(ym, z), at_yz(y, zp), at_yz(y, zm)
    d_z1, d_z3 = at_yz(y, z + 1 - 2 * (z % 2)), at_yz(y, 3 - z)
    d_y1, d_y3 = at_yz(y + 1 - 2 * (y % 2), z), at_yz(3 - y, z)

    def rc(src, dst, k, dev):
        return pltpu.make_async_remote_copy(
            src_ref=src, dst_ref=dst, send_sem=ssem.at[k], recv_sem=rsem.at[k],
            device_id=dev, device_id_type=MESH,
        )

    def go(copies):
        for cp in copies:
            cp.start()

    def done(copies):
        for cp in copies:
            cp.wait()

    def lane(q, base):
        return pl.ds(pl.multiple_of(base + 128 * q, 128), 128)

    left, right = pl.ds(0, TOK), pl.ds(TOK, TOK)
    ca = pl.ds(0, HALF)
    tok_rows, dy_rows, meta_rows = pl.ds(0, FEAT), pl.ds(FEAT, FEAT), pl.ds(2 * FEAT, 16)

    own = [
        pltpu.make_async_copy(routes_h, rbuf, lsem.at[0]),
        pltpu.make_async_copy(gates_h, gbuf, lsem.at[1]),
        pltpu.make_async_copy(tok_h, gat.at[0, tok_rows, left], lsem.at[2]),
        pltpu.make_async_copy(dy_h, gat.at[0, dy_rows, left], lsem.at[3]),
    ]
    go(own)
    weights = [pltpu.make_async_copy(h, wt.at[m], lsem.at[4 + m]) for m, h in enumerate((wg_h, wu_h, wd_h))]
    go(weights[:1])
    barrier = pltpu.get_barrier_semaphore()
    for dev in (mate, xpd, xmd, ypd, ymd, zpd, zmd):
        pl.semaphore_signal(barrier, inc=1, device_id=dev, device_id_type=MESH)
    done(own[:2])
    gat[0, meta_rows, left] = jnp.concatenate([rbuf[...].astype(F32), gbuf[...].astype(F32)], 0).astype(BF)
    row_i = lax.broadcasted_iota(jnp.int32, (TOK, TOK), 0)
    col_i = lax.broadcasted_iota(jnp.int32, (TOK, TOK), 1)
    tri[...] = jnp.where(row_i < col_i, 1.0, 0.0).astype(BF)
    done(own[2:])
    go(weights[1:])
    pl.semaphore_wait(barrier, 7)
    first = [
        rc(gat.at[0, :, left], gat.at[0, :, right], 0, mate),
        rc(gat.at[0, :, left], gat.at[3, :, left], 1, xpd),
        rc(gat.at[0, :, left], gat.at[1, :, left], 2, xmd),
    ]
    second = [
        rc(gat.at[3, tok_rows, left], gat.at[2, tok_rows, left], 3, xpd),
        rc(gat.at[1, pl.ds(FEAT, BLK - FEAT), left], gat.at[2, pl.ds(FEAT, BLK - FEAT), left], 4, xmd),
        rc(gat.at[3, :, left], gat.at[3, :, right], 5, mate),
        rc(gat.at[1, :, left], gat.at[1, :, right], 6, mate),
    ]
    third = [rc(gat.at[2, :, left], gat.at[2, :, right], 7, mate)]
    go(first)

    def bufs(par):
        return (prt.at[par], r1a, r1b, r2a, r2b, sa, sb, r3a, r3b, r4a, r4b, act.at[par])

    half_bufs = (prt_h, r1a_h, r1b_h, r2a_h, r2b_h, sa_h, sb_h, r3a_h, r3b_h, r4a_h, r4b_h, act_h)
    k0 = Part(0, (0, CAPS), (0, TOK), CAPS, NLO, bufs(0), 20, 0, 0)
    k1 = Part(3, (0, ROWS), (0, PAIR), ROWS, CAPS, bufs(1), 20, 1, 1)
    k2 = Part(2, (0, ROWS), (0, PAIR), ROWS, CAPS, bufs(0), 20, 0, 0)
    k3 = Part(1, (0, ROWS), (0, PAIR), ROWS, CAPS, bufs(1), 20, 1, 1)
    kh = Part(0, (CAPS, ROWS), (TOK, PAIR), CAPS, NLO, half_bufs, 80, 0, 2)

    def meta_of(k):
        m = gat[k.r, meta_rows, k.ln].astype(F32)
        return m[:8], m[8:]

    def expert_id(e):
        return (node * EXP + e).astype(F32)

    def slot_rows(k):
        routes, _ = meta_of(k)
        wide = (16, k.width)
        rid = lax.broadcasted_iota(jnp.int32, wide, 0)
        member = jnp.zeros(wide, F32)
        for e in range(EXP):
            one = jnp.sum(jnp.where(routes == expert_id(e), 1.0, 0.0), axis=0, keepdims=True)
            member = jnp.where(rid == e, jnp.broadcast_to(one, wide), member)
        for h in range(k.width // TOK):
            mine = member[:, h * TOK : (h + 1) * TOK]
            before = dot_n(mine.astype(BF), tri[...])
            slot[:, pl.ds(h * TOK, TOK)] = jnp.where(mine > 0.5, before + float(CAPS * h), -1.0)
        sid = lax.broadcasted_iota(jnp.int32, (k.n, k.width), 0).astype(F32)

        def rows_of(e, carry):
            o = jnp.where(sid == slot[pl.ds(e, 1), pl.ds(0, k.width)], 1.0, 0.0).astype(BF)
            hot[k.r, e, k.rw, k.ln] = o
            xb[0, e, k.rw] = dot_t(o, gat[k.r, tok_rows, k.ln]).astype(BF)
            xb[1, e, k.rw] = dot_t(o, gat[k.r, dy_rows, k.ln]).astype(BF)
            return carry

        lax.fori_loop(0, EXP, rows_of, 0)

    def project(k):
        slot_rows(k)

        def products(e, carry):
            for m in range(3):
                k.p[m, e, k.all] = dot_n(xb[m // 2, e, k.rw], wt[m, e]).astype(BF)
            return carry

        lax.fori_loop(0, EXP, products, 0)

    def half_product(k):
        def one_half(j, carry):
            e = (y2 + j) % 4
            for m in range(3):
                k.p[m, e, k.all, ca] = dot_n(xb[m // 2, e, k.rw], wt[m, e, :, ca]).astype(BF)
            return carry

        return one_half

    def first_products(k):
        at = lane(z2, HALF)
        lax.fori_loop(0, 1, half_product(k), 0)

        def one_column(e, carry):
            for m in range(3):
                k.p[m, e, k.all, at] = dot_n(xb[m // 2, e, k.rw], wt[m, e, :, at]).astype(BF)
            return carry

        lax.fori_loop(0, EXP, one_column, 0)

    def rest_products(k):
        lax.fori_loop(1, EXP, half_product(k), 0)

        def other_columns(e, carry):
            for m in range(3):
                tb[m, k.all] = dot_n(xb[m // 2, e, k.rw], wt[m, e, :, pl.ds(HALF, HALF)]).astype(BF)
            for m in range(3):
                for j in range(1, 4):
                    q = (z2 + j) % 4
                    k.p[m, e, k.all, lane(q, HALF)] = tb[m, k.all, lane(q, 0)]
            return carry

        lax.fori_loop(0, EXP, other_columns, 0)

    def s1(k):
        p, b = k.p, k.base
        return [
            rc(p.at[:, y2, k.lo, ca], k.r1a.at[0, :, k.nlo], b, ymd),
            rc(p.at[:, y2, k.hi, ca], k.r1a.at[1, :, k.nhi], b + 1, ypd),
            rc(p.at[:, :, k.lo, lane(z2, HALF)], k.r1b.at[0, :, :, k.nlo], b + 2, zmd),
            rc(p.at[:, :, k.hi, lane(z2, HALF)], k.r1b.at[1, :, :, k.nhi], b + 3, zpd),
        ]

    def s1_add(k):
        p = k.p
        for m in range(3):
            p[m, ym, k.lo, ca] = add2(p[m, ym, k.lo, ca], k.r1a[0, m, k.nlo])
            p[m, yp, k.hi, ca] = add2(p[m, yp, k.hi, ca], k.r1a[1, m, k.nhi])
            p[m, :, k.lo, lane(zm, HALF)] = add2(p[m, :, k.lo, lane(zm, HALF)], k.r1b[0, m, :, k.nlo])
            p[m, :, k.hi, lane(zp, HALF)] = add2(p[m, :, k.hi, lane(zp, HALF)], k.r1b[1, m, :, k.nhi])

    def s2(k, g):
        p, b, ms = k.p, k.base + 4 + 4 * g, (pl.ds(0, 1), pl.ds(1, 2))[g]
        return [
            rc(p.at[ms, yp, k.all, ca], k.r2a.at[0, ms, k.all], b, ypd),
            rc(p.at[ms, ym, k.all, ca], k.r2a.at[1, ms, k.all], b + 1, ymd),
            rc(p.at[ms, :, k.all, lane(zp, HALF)], k.r2b.at[0, ms, :, k.all], b + 2, zpd),
            rc(p.at[ms, :, k.all, lane(zm, HALF)], k.r2b.at[1, ms, :, k.all], b + 3, zmd),
        ]

    def s2_add(k):
        p = k.p
        for m in range(3):
            k.sa[m, k.all] = add3(p[m, y, k.all, ca], k.r2a[0, m, k.all], k.r2a[1, m, k.all]).astype(BF)
            k.sb[m, :, k.all] = add3(
                p[m, :, k.all, lane(z, HALF)], k.r2b[0, m, :, k.all], k.r2b[1, m, :, k.all]
            ).astype(BF)

    def s3(k):
        b = k.base + 12
        return [
            rc(k.sa.at[:, k.lo, lane(z2, 0)], k.r3a.at[0, :, k.nlo], b, zmd),
            rc(k.sa.at[:, k.hi, lane(z2, 0)], k.r3a.at[1, :, k.nhi], b + 1, zpd),
            rc(k.sb.at[:, y2, k.lo], k.r3b.at[0, :, k.nlo], b + 2, ymd),
            rc(k.sb.at[:, y2, k.hi], k.r3b.at[1, :, k.nhi], b + 3, ypd),
        ]

    def s3_add(k):
        a, b = k.sa, k.sb
        for m in range(3):
            a[m, k.lo, lane(zm, 0)] = add2(a[m, k.lo, lane(zm, 0)], k.r3a[0, m, k.nlo])
            a[m, k.hi, lane(zp, 0)] = add2(a[m, k.hi, lane(zp, 0)], k.r3a[1, m, k.nhi])
            b[m, ym, k.lo] = add2(b[m, ym, k.lo], k.r3b[0, m, k.nlo])
            b[m, yp, k.hi] = add2(b[m, yp, k.hi], k.r3b[1, m, k.nhi])

    def s4(k):
        b = k.base + 16
        return [
            rc(k.sa.at[:, k.all, lane(zp, 0)], k.r4a.at[0, :, k.all], b, zpd),
            rc(k.sa.at[:, k.all, lane(zm, 0)], k.r4a.at[1, :, k.all], b + 1, zmd),
            rc(k.sb.at[:, yp, k.all], k.r4b.at[0, :, k.all], b + 2, ypd),
            rc(k.sb.at[:, ym, k.all], k.r4b.at[1, :, k.all], b + 3, ymd),
        ]

    def activate(k):
        routes, gates = meta_of(k)
        match = jnp.where(routes == expert_id(y), 1.0, 0.0)
        gate_row = jnp.sum(match * gates, axis=0, keepdims=True)
        oh = hot[k.r, y, k.rw, k.ln].astype(F32)
        q = jnp.sum(oh * gate_row, axis=1, keepdims=True)
        dots = jnp.zeros((k.n, 1), F32)
        for h in range(2):
            if h == 0:
                g, u, b = (
                    add3(k.sa[m, k.all, lane(z, 0)], k.r4a[0, m, k.all], k.r4a[1, m, k.all]) for m in range(3)
                )
            else:
                g, u, b = (add3(k.sb[m, y, k.all], k.r4b[0, m, k.all], k.r4b[1, m, k.all]) for m in range(3))
            logistic = 1.0 / (1.0 + jnp.exp(-g))
            swished = g * logistic
            hidden = swished * u
            dots = dots + jnp.sum(hidden * b, axis=1, keepdims=True)
            scaled = q * b
            at = lane(z, h * HALF)
            k.t[0, y, k.all, at] = (scaled * u * logistic * (1.0 + g * (1.0 - logistic))).astype(BF)
            k.t[1, y, k.all, at] = (scaled * swished).astype(BF)
            k.t[2, y, k.all, at] = (q * hidden).astype(BF)
        dv[k.d, 0, :, pl.ds(0, k.width)] = match * jnp.sum(oh * dots, axis=0, keepdims=True)

    def share(k, step, b, dev):
        at = pl.ds(0, k.width)
        return rc(dv.at[k.d, step, :, at], dr.at[k.d, step, :, at], b, dev)

    def a1(k):
        t, b = k.t, k.base + 20
        az, bz = t.at[:, y, k.all, lane(z, 0)], t.at[:, y, k.all, lane(z, HALF)]
        return [rc(az, az, b, zpd), rc(az, az, b + 1, zmd), rc(bz, bz, b + 2, ypd), rc(bz, bz, b + 3, ymd),
                share(k, 0, b + 4, d_z1)]

    def a2(k):
        t, b = k.t, k.base + 25
        v = [t.at[:, y, k.lo, lane(zm, 0)], t.at[:, y, k.hi, lane(zp, 0)],
             t.at[:, ym, k.lo, lane(z, HALF)], t.at[:, yp, k.hi, lane(z, HALF)]]
        return [rc(v[0], v[0], b, zpd), rc(v[1], v[1], b + 1, zmd), rc(v[2], v[2], b + 2, ypd),
                rc(v[3], v[3], b + 3, ymd), share(k, 1, b + 4, d_z3)]

    def a3(k, g):
        t, b, ms = k.t, k.base + 30 + 4 * g, (pl.ds(0, 2), pl.ds(2, 1))[g]
        ay, bz = t.at[ms, y, k.all, ca], t.at[ms, :, k.all, lane(z, HALF)]
        own_share = [share(k, 2, b + 4, d_y1)] if g else []
        return [rc(ay, ay, b, ypd), rc(ay, ay, b + 1, ymd), rc(bz, bz, b + 2, zpd), rc(bz, bz, b + 3, zmd),
                *own_share]

    def a4(k, g):
        t, b, ms = k.t, k.base + 39 + 9 * k.par + 4 * g, (pl.ds(0, 2), pl.ds(2, 1))[g]
        v = [t.at[ms, ym, k.lo, ca], t.at[ms, yp, k.hi, ca],
             t.at[ms, :, k.lo, lane(zm, HALF)], t.at[ms, :, k.hi, lane(zp, HALF)]]
        own_share = [share(k, 3, b + 4, d_y3)] if g else []
        return [rc(v[0], v[0], b, ypd), rc(v[1], v[1], b + 1, ymd), rc(v[2], v[2], b + 2, zpd),
                rc(v[3], v[3], b + 3, zmd), *own_share]

    def dstep(k, step):
        at = pl.ds(0, k.width)
        dv[k.d, step + 1, :, at] = dv[k.d, step, :, at] + dr[k.d, step, :, at]

    def do_s1(k):
        done(s1(k))
        s1_add(k)
        go(s2(k, 0))
        go(s2(k, 1))

    def do_s2(k):
        done(s2(k, 0))
        done(s2(k, 1))
        s2_add(k)
        go(s3(k))

    def do_s3(k):
        done(s3(k))
        s3_add(k)
        go(s4(k))

    def do_a1(k):
        done(a1(k))
        dstep(k, 0)
        go(a2(k))

    def do_a2(k):
        done(a2(k))
        dstep(k, 1)
        go(a3(k, 0))

    def do_a3(k):
        done(a3(k, 0))
        done(a3(k, 1))
        dstep(k, 2)

    def arrive(k):
        done(a4(k, 0))
        done(a4(k, 1))
        dstep(k, 3)

    def post_a(k, start=0, size=FEAT, between=None):
        at, fr = pl.ds(0, k.width), pl.ds(start, size)
        bk[fr, at] = jnp.zeros((size, k.width), F32)

        def one_expert(e, carry):
            rb = dot_t(wt[0, e, fr], k.t[0, e, k.all]) + dot_t(wt[1, e, fr], k.t[1, e, k.all])
            bk[fr, at] += dot_n(rb.astype(BF), hot[k.r, e, k.rw, k.ln])
            return carry

        if between is None:
            lax.fori_loop(0, EXP, one_expert, 0)
        else:
            lax.fori_loop(0, EXP // 2, one_expert, 0)
            between()
            lax.fori_loop(EXP // 2, EXP, one_expert, 0)
        cb[k.r, fr, k.ln] = bk[fr, at].astype(BF)
        if start + size == FEAT:
            cb[k.r, pl.ds(FEAT, 16), k.ln] = jnp.concatenate(
                [dv[k.d, 4, :, at], jnp.zeros((8, k.width), F32)], 0
            ).astype(BF)

    def post_b(k, fresh=False):
        def one_expert(e, carry):
            xt = dot_t(gat[k.r, tok_rows, k.ln], hot[k.r, e, k.rw, k.ln]).astype(BF)
            gr = dot_t(gat[k.r, dy_rows, k.ln], hot[k.r, e, k.rw, k.ln]).astype(BF)
            for m, side in enumerate((xt, xt, gr)):
                new = dot_n(side, k.t[m, e, k.all])
                acc[m][e] = (new if fresh else acc[m][e].astype(F32) + new).astype(BF)
            return carry

        lax.fori_loop(0, EXP, one_expert, 0)

    def c1(r):
        return [rc(cb.at[r, :, right], c1r.at[r], 8 + r, mate)]

    def do_c1(r):
        done(c1(r))
        cs[r] = add2(cb[r, :, left], c1r[r])

    top, low = pl.ds(0, CUT), pl.ds(CUT, CROWS - CUT)
    c2 = [rc(cs.at[2, top], c2a, 12, xpd), rc(cs.at[2, low], c2b, 13, xmd)]
    c1_last = [rc(cb.at[1, top, right], c1r.at[1, top], 9, mate), rc(cb.at[1, low, right], c1r.at[1, low], 16, mate)]
    c3 = [
        rc(cs.at[1, top], c3r.at[0, top], 14, xpd),
        rc(cs.at[1, low], c3r.at[0, low], 17, xpd),
        rc(cs.at[3], c3r.at[1], 15, xmd),
    ]

    def count_loads():
        eid = lax.broadcasted_iota(jnp.int32, (1, ALL_EXPERTS), 1)
        ld[...] = jnp.zeros_like(ld)

        def one_block(b, carry):
            r = (b // 2 - x + 4) % 4
            cc = (b % 2 + c) % 2
            m = gat[r, meta_rows, pl.ds(pl.multiple_of(cc * TOK, TOK), TOK)].astype(F32)
            routes, gates = m[:8], m[8:]
            tot = jnp.zeros((1, ALL_EXPERTS), F32)
            for e in range(ALL_EXPERTS):
                v = jnp.sum(jnp.where(routes == float(e), gates, 0.0), axis=0, keepdims=True)
                v = jnp.sum(v, axis=1, keepdims=True)
                tot = jnp.where(eid == e, jnp.broadcast_to(v, (1, ALL_EXPERTS)), tot)
            ld[...] += tot
            return carry

        lax.fori_loop(0, 8, one_block, 0)
        ld[...] = ld[...] * (1.0 / 64.0)

    slot_rows(k0)
    done(weights)
    first_products(k0)
    go(s1(k0))
    done(first[:1])
    slot_rows(kh)
    first_products(kh)
    go(s1(kh))
    rest_products(k0)
    do_s1(k0)
    rest_products(kh)
    done(first[1:])
    go(second)
    do_s1(kh)
    done(second[2:3])
    project(k1)
    do_s2(k0)
    go(s1(k1))
    do_s2(kh)
    do_s3(k0)
    done(second[:2])
    done(second[3:])
    go(third)
    done(s1(k1))
    s1_add(k1)
    go(s2(k1, 0))
    done(s4(k0))
    activate(k0)
    go(a1(k0))
    do_s3(kh)
    go(s2(k1, 1))

    done(third)
    count_loads()
    project(k2)
    do_a1(k0)
    done(s4(kh))
    activate(kh)
    go(a1(kh))
    do_s2(k1)
    do_a2(k0)
    go(a3(k0, 1))
    do_s3(k1)
    go(s1(k2))
    done(s4(k1))
    activate(k1)
    go(a1(k1))

    done(s1(k2))
    s1_add(k2)
    go(s2(k2, 0))
    do_a3(k0)
    go(a4(k0, 0))
    go(a4(k0, 1))
    do_a1(k1)
    go(s2(k2, 1))
    do_a2(k1)
    arrive(k0)
    post_a(k0)
    post_b(k0, True)
    do_s2(k2)
    go(a3(k1, 1))
    project(k3)
    do_s3(k2)
    go(s1(k3))
    do_a3(k1)
    do_a1(kh)
    done(s4(k2))
    activate(k2)
    go(a1(k2))
    go(a4(k1, 0))
    go(a4(k1, 1))

    done(s1(k3))
    s1_add(k3)
    go(s2(k3, 0))
    do_a1(k2)
    go(s2(k3, 1))
    do_a2(k2)
    arrive(k1)
    post_a(k1)
    go(c1(3))
    post_b(k1)
    do_s2(k3)
    go(a3(k2, 1))
    do_s3(k3)
    do_a3(k2)
    go(a4(k2, 0))
    go(a4(k2, 1))
    done(s4(k3))
    activate(k3)
    go(a1(k3))

    do_a2(kh)
    go(a3(kh, 1))
    do_c1(3)
    do_a1(k3)
    do_a3(kh)
    go(a4(kh, 0))
    go(a4(kh, 1))
    do_a2(k3)
    go(a3(k3, 1))
    arrive(k2)
    post_a(k2)
    go(c1(2))
    post_b(k2)
    do_c1(2)
    go(c2)
    done(a3(k3, 0))
    go(a4(k3, 0))
    arrive(kh)
    post_a(kh)
    go(c1(0))
    done(a3(k3, 1))
    dstep(k3, 2)
    go(a4(k3, 1))
    done(c2)
    cs[3, low, :] = add2(cs[3, low, :], c2b[...])
    c3[2].start()
    post_b(kh)
    do_c1(0)
    done(a4(k3, 0))
    post_a(k3, 0, CUT)
    c1_last[0].start()
    done(a4(k3, 1))
    dstep(k3, 3)

    def send_top():
        c1_last[0].wait()
        cs[1, top, :] = add3(cb[1, top, left], c1r[1, top], c2a[...]).astype(BF)
        c3[0].start()

    post_a(k3, CUT, FEAT - CUT, send_top)
    c1_last[1].start()
    c1_last[1].wait()
    cs[1, low, :] = add2(cb[1, low, left], c1r[1, low])
    c3[1].start()
    post_b(k3)
    c3[2].wait()
    c3[0].wait()
    gt[top, :] = add3(cs[0, top], c3r[0, top], c3r[1, top]).astype(BF)
    c3[1].wait()
    rest = add3(cs[0, low], c3r[0, low], c3r[1, low])
    gt[pl.ds(CUT, FEAT - CUT), :] = rest[: FEAT - CUT].astype(BF)
    gg[...] = rest[FEAT - CUT : FEAT - CUT + 8].astype(BF)


def flush(g0, g1, g2, g3, g4, g5, o0, o1, o2, o3, o4, o5, sem):
    copies = [
        pltpu.make_async_copy(a, b, sem.at[n])
        for n, (a, b) in enumerate(((g3, o3), (g4, o4), (g5, o5), (g0, o0), (g1, o1), (g2, o2)))
    ]
    for cp in copies:
        cp.start()
    for cp in copies:
        cp.wait()


def on_device(tokens, grad_out, gates, routes, w_gate, w_up, w_down):
    any_ = pl.BlockSpec(memory_space=pl.ANY)
    V = pltpu.VMEM
    w_shape = (EXP, FEAT, HID)

    def comm(copies, rows, cut):
        lead = () if copies is None else (copies,)
        return [
            V((*lead, 3, EXP, rows, HID), BF),
            V((2, 3, cut, HALF), BF), V((2, 3, EXP, cut, 128), BF),
            V((2, 3, rows, HALF), BF), V((2, 3, EXP, rows, 128), BF),
            V((3, rows, HALF), BF), V((3, EXP, rows, 128), BF),
            V((2, 3, cut, 128), BF), V((2, 3, cut, 128), BF),
            V((2, 3, rows, 128), BF), V((2, 3, rows, 128), BF),
            V((*lead, 3, EXP, rows, HID), BF),
        ]

    scratch = [
        V((3, *w_shape), BF), V((4, BLK, PAIR), BF), V((TOK, TOK), BF), V((4, EXP, ROWS, PAIR), BF),
        V((16, PAIR), F32), V((2, EXP, ROWS, FEAT), BF), V((3, CAPS, HALF), BF),
        V((8, TOK), jnp.int32), V((8, TOK), BF),
        *comm(2, ROWS, CAPS), *comm(None, CAPS, NLO),
        V((3, 5, 8, PAIR), F32), V((3, 4, 8, PAIR), F32), V((2, 8, PAIR), F32),
        V((FEAT, PAIR), F32), V((4, CROWS, PAIR), BF), V((4, CROWS, TOK), BF),
        V((4, CROWS, TOK), BF), V((CUT, TOK), BF), V((CROWS - CUT, TOK), BF), V((2, CROWS, TOK), BF),
        pltpu.SemaphoreType.DMA((7,)), pltpu.SemaphoreType.DMA((128,)), pltpu.SemaphoreType.DMA((128,)),
    ]
    results = pl.pallas_call(
        kernel,
        name="expert_backward",
        out_shape=(
            V((FEAT, TOK), BF), V((8, TOK), BF), V((1, ALL_EXPERTS), F32),
            V(w_shape, BF), V(w_shape, BF), V(w_shape, BF),
        ),
        in_specs=[any_] * 7,
        out_specs=[pl.BlockSpec(memory_space=pltpu.VMEM)] * 6,
        scratch_shapes=scratch,
        compiler_params=pltpu.CompilerParams(
            collective_id=0, has_side_effects=True, vmem_limit_bytes=54_400_000
        ),
    )(routes.T, gates.T, tokens.T, grad_out.T, w_gate, w_up, jnp.transpose(w_down, (0, 2, 1)))
    shape = jax.ShapeDtypeStruct
    gt, gg, ld, og, ou, od = pl.pallas_call(
        flush,
        name="write_results",
        out_shape=(
            shape((FEAT, TOK), BF), shape((8, TOK), BF), shape((1, ALL_EXPERTS), F32),
            shape(w_shape, BF), shape(w_shape, BF), shape(w_shape, BF),
        ),
        in_specs=[pl.BlockSpec(memory_space=pltpu.VMEM)] * 6,
        out_specs=[any_] * 6,
        scratch_shapes=[pltpu.SemaphoreType.DMA((6,))],
        compiler_params=pltpu.CompilerParams(vmem_limit_bytes=8_000_000),
    )(*results)
    return gt.T, gg.T, og, ou, jnp.transpose(od, (0, 2, 1)), ld.reshape(ALL_EXPERTS)


def solution(mesh):
    in_specs = (
        P("node", "local"),
        P("node", "local"),
        P("node", None),
        P("node", None),
        P("node", "local", None),
        P("node", "local", None),
        P("node", None, "local"),
    )
    out_specs = (
        P("node", "local"),
        P("node", None),
        P("node", "local", None),
        P("node", "local", None),
        P("node", None, "local"),
        P(),
    )
    return jax.shard_map(
        on_device, mesh=mesh, in_specs=in_specs, out_specs=out_specs, check_vma=False
    )
```
